32 devices in a mesh: depth: 2 (over y), azim: 16 (over z, x, core).
Axes of the slice: x: 2, y: 2, z: 4, core: 2. Of those that a mesh axis runs over, the one named last changes fastest.
Arguments:
- cotangent: bfloat16 [128, 4096, 256], P('depth', 'azim'), may hold values from -6 to 6
- pre_second: bfloat16 [128, 4096, 256], P('depth', 'azim'), may hold values from -6 to 6
- pre_first: bfloat16 [128, 4096, 256], P('depth', 'azim'), may hold values from -6 to 6
- kernel_first: bfloat16 [3, 3, 3, 32, 32], replicated, may hold values from -0.21875 to 0.21875
- kernel_second: bfloat16 [3, 3, 3, 32, 32], replicated, may hold values from -0.21875 to 0.21875
- row_resample: float32 [4, 128, 8, 8], P(None, 'depth'), may hold values from -0.1875 to 0.1875
- col_taps: float32 [4, 128, 8], P(None, 'depth'), may hold values from 0.1 to 1
- band_width: int32 [4, 128], P(None, 'depth'), may hold values from 1 to 8
- col_offset: int32 [4, 128], P(None, 'depth'), may hold values from -24 to 24, as said below
Outputs:
- cam_grad: float32 [8, 4096, 128], P('depth', 'azim')
The draws below stay inside these ranges and needn't reach their ends.
Inputs may be any that keep to these rules, and one draw needn't show every extreme that they name: `col_offset`: some entry equals -24 and some entry equals 24.
All inputs are finite; a program needn't handle non-finite values.
Results may differ from the reference program's by a relative error of at most 0.0048.
Values may be sent and summed in bfloat16 or wider, within the bound.
No kernel may reach another device: no remote copies, remote signals or barrier semaphores. Data moves between devices by JAX's collectives and lax.ppermute only.
A program may use at most 256 MiB of HBM per device.

```python
import math
import jax
import jax.numpy as jnp
from jax import lax

C = 32
DEPTH = 128
AZIM = 4096
CAMS = 4
TAPS = 8
SHIFT = 24
ROWS = 8


def draw_col_offset(key, part):
    key_base, key_cam_low, key_sphere, key_cam_high = jax.random.split(jax.random.fold_in(key, 17), 4)
    offsets = jax.random.randint(key_base, (CAMS, DEPTH), -SHIFT, SHIFT + 1, dtype=jnp.int32)
    camera_low = jax.random.randint(key_cam_low, (), 0, CAMS, dtype=jnp.int32)
    sphere_low = jax.random.randint(key_sphere, (), 0, DEPTH, dtype=jnp.int32)
    camera_high = jax.random.randint(key_cam_high, (), 0, CAMS, dtype=jnp.int32)
    offsets = offsets.at[camera_low, sphere_low].set(-SHIFT)
    offsets = offsets.at[camera_high, (sphere_low + 1) % DEPTH].set(SHIFT)
    return offsets


def touch_ends(values, rng, low, largest):
    dims = values.shape
    place = [jax.random.randint(jax.random.fold_in(rng, axis), (), 0, dims[axis]) for axis in range(len(dims))]
    values = values.at[tuple(place)].set(low)
    longest = dims.index(max(dims))
    place[longest] = (place[longest] + 1) % dims[longest]
    return values.at[tuple(place)].set(largest)


def levels(stream_key, extent, pieces, least, top_value):
    level = 1.0
    for dim, blocks in pieces:
        heights = jax.random.uniform(jax.random.fold_in(jax.random.fold_in(stream_key, 6), dim), (blocks,), jnp.float32, least / len(pieces), top_value / len(pieces))
        level = level * jnp.repeat(jnp.exp(heights), extent[dim] // blocks).reshape((-1,) + (1,) * (len(extent) - 1 - dim))
    return level


def normal_values(own_key, shape, deviation, reach, shards=(), kind=jnp.bfloat16):
    gain = levels(own_key, shape, shards, -0.22, 0.18) if shards else 1.0
    entries = jax.random.normal(own_key, shape, jnp.float32) * deviation * gain
    return jnp.minimum(jnp.maximum(entries, -reach), reach).astype(kind)


def setup_inputs(seed: int = 0) -> dict:
    key_of = jax.random.split(jax.random.key(seed), 10)
    return {
        "cotangent": normal_values(key_of[0], (DEPTH, AZIM, ROWS * C), 1.0, 6.0, ((0, 2), (1, 16))),
        "pre_second": normal_values(key_of[1], (DEPTH, AZIM, ROWS * C), 1.0, 6.0, ((0, 2), (1, 16))),
        "pre_first": normal_values(key_of[2], (DEPTH, AZIM, ROWS * C), 1.0, 6.0, ((0, 2), (1, 16))),
        "kernel_first": normal_values(key_of[3], (3, 3, 3, C, C), (27 * C) ** -0.5, 0.21875),
        "kernel_second": normal_values(key_of[4], (3, 3, 3, C, C), (27 * C) ** -0.5, 0.21875),
        "row_resample": normal_values(key_of[5], (CAMS, DEPTH, ROWS, ROWS), (ROWS * DEPTH) ** -0.5, 0.1875, ((1, 2),), jnp.float32),
        "col_taps": jnp.clip(0.1 + 0.9 * jax.random.uniform(key_of[6], (CAMS, DEPTH, TAPS), jnp.float32) ** levels(key_of[6], (CAMS, DEPTH, TAPS), ((1, 2),), -0.2, 0.2), 0.1, 1.0),
        "band_width": touch_ends(jax.random.randint(key_of[7], (CAMS, DEPTH), 1, TAPS + 1), jax.random.fold_in(key_of[7], 1), 1, TAPS).astype(jnp.int32),
        "col_offset": draw_col_offset(jax.random.fold_in(key_of[9], 71), 0),
    }


def transpose_conv(grad, kernel):
    sphere_count, column_count, row_count, channels = grad.shape
    wrapped = jnp.concatenate([grad[:, -1:], grad, grad[:, :1]], axis=1)
    padded = jnp.pad(wrapped, ((1, 1), (0, 0), (1, 1), (0, 0)))
    flipped = jnp.transpose(kernel[::-1, ::-1, ::-1], (0, 1, 2, 4, 3)).astype(jnp.float32)
    blocksize = math.gcd(sphere_count, 8)

    def one_block(start):
        piece = lax.dynamic_slice_in_dim(padded, start, blocksize + 2, 0).astype(jnp.float32)
        result = lax.conv_general_dilated(piece[None], flipped, (1, 1, 1), "VALID",
                                          dimension_numbers=("NDHWC", "DHWIO", "NDHWC"),
                                          precision=lax.Precision.HIGHEST)
        return result[0]

    starts = jnp.arange(sphere_count // blocksize, dtype=jnp.int32) * blocksize
    return lax.map(one_block, starts).reshape(sphere_count, column_count, row_count, channels)


def reference(cotangent, pre_second, pre_first, kernel_first, kernel_second, row_resample, col_taps, band_width, col_offset):
    layout = (DEPTH, AZIM, ROWS, C)
    second_grad = jnp.where(pre_second > 0, cotangent, jnp.zeros_like(cotangent)).reshape(layout)
    hidden_grad = transpose_conv(second_grad, kernel_second)
    gate_first = (pre_first.reshape(layout) > 0).astype(jnp.float32)
    first_grad = (hidden_grad * gate_first).astype(jnp.bfloat16)
    volume_grad = transpose_conv(first_grad, kernel_first).astype(jnp.bfloat16)
    band_keep = lax.broadcasted_iota(jnp.int32, col_taps.shape, 2) < band_width[:, :, None]
    band_taps = jnp.where(band_keep, col_taps, jnp.zeros_like(col_taps)).astype(jnp.bfloat16)
    columns = jnp.arange(AZIM, dtype=jnp.int32)
    results = []
    for camera in range(CAMS):
        def step(accumulated, inputs):
            plane, taps_now, offset_now, resample = inputs
            pulled = jnp.zeros((AZIM, ROWS, C), jnp.float32)
            for tap in range(TAPS):
                source = ((columns + offset_now + tap) % AZIM).astype(jnp.int32)
                pulled = pulled + taps_now[tap].astype(jnp.float32) * jnp.take(plane, source, axis=0).astype(jnp.float32)
            accumulated = accumulated + jnp.einsum("hg,whc->gwc", resample, pulled, precision=lax.Precision.HIGHEST)
            return accumulated, None

        start = jnp.zeros((ROWS, AZIM, C), jnp.float32)
        accumulated, unused = lax.scan(step, start, (volume_grad, band_taps[camera], col_offset[camera], row_resample[camera]))
        results.append(accumulated)
    return jnp.concatenate(results, axis=-1)
```

```python
import functools

import jax
import jax.numpy as jnp
from jax import lax
from jax.experimental import pallas as pl
from jax.experimental.pallas import tpu as pltpu
from jax.sharding import PartitionSpec as P

TAPS = 8
SHIFT = 24
MARGIN = SHIFT + TAPS
GROUP = 4
VBLOCK = 64
BF16 = jnp.bfloat16
F32 = jnp.float32


def sweep_kernel(
    sphere_rim,
    column_rim,
    cot_a,
    cot_b,
    cot_zero,
    second_a,
    second_b,
    second_zero,
    first_a,
    first_b,
    first_c,
    first_d,
    first_zero,
    mixer_second,
    mixer_first,
    resample,
    bands,
    out_ref,
    taps_one,
    taps_two,
    padded_one,
    padded_two,
    volume,
    mixed,
    total,
):
    step = pl.program_id(0)
    steps = pl.num_programs(0)
    last = step == steps - 1
    columns, merged = cot_a.shape[1:]
    cameras, row_count = resample.shape[1:3]
    channels = merged // row_count
    wide = columns + 16
    blocks = columns // VBLOCK
    window = VBLOCK + 2 * MARGIN

    def store_taps(source, target, slot, rows):
        for tap in range(3):
            target[slot, :, tap * merged : (tap + 1) * merged] = source[
                9 - tap : 9 - tap + rows
            ].astype(BF16)

    def gate_second(grad, index, sphere, slot):
        padded = padded_one.at[index]
        padded[16 : 16 + columns] = grad.astype(F32)
        padded[8:16] = column_rim[sphere, 0:8].astype(F32)
        padded[16 + columns : 24 + columns] = column_rim[sphere, 8:16].astype(F32)
        store_taps(padded, taps_one, slot, wide)

    def masked(cot, saved):
        return jnp.where(saved > 0, cot, jnp.zeros_like(cot))

    def conv(source, mixers, slots):
        lhs = lambda depth: jnp.concatenate(
            [source[slot + 2 - depth] for slot in slots], axis=0
        )
        value = jnp.dot(lhs(2), mixers[2], preferred_element_type=F32)
        value = value + jnp.dot(lhs(1), mixers[1], preferred_element_type=F32)
        return value + jnp.dot(lhs(0), mixers[0], preferred_element_type=F32)

    def gate_first(hidden, saved, index, sphere, slot):
        low = column_rim[sphere, 16:24].astype(F32)
        high = column_rim[sphere, 24:32].astype(F32)
        keep = jnp.concatenate([low, saved.astype(F32), high], axis=0) > 0
        padded_two[index] = jnp.where(keep, hidden, 0.0)
        store_taps(padded_two.at[index], taps_two, slot, columns)

    lane = lax.broadcasted_iota(jnp.int32, (channels, merged), 1)
    diagonal = lax.rem(lane, channels) == lax.broadcasted_iota(
        jnp.int32, (channels, merged), 0
    )

    def mix_rows(group):
        for camera in range(cameras):
            for sphere in range(GROUP):
                rows = resample[group * GROUP + sphere, camera]
                weights = jnp.concatenate(
                    [jnp.where(diagonal, rows[r : r + 1], 0.0) for r in range(row_count)],
                    axis=0,
                ).astype(BF16)
                value = jnp.dot(
                    volume[sphere], weights, preferred_element_type=F32
                ).astype(BF16)
                for block in range(blocks):
                    mixed[camera, block, sphere * VBLOCK : (sphere + 1) * VBLOCK] = value[
                        block * VBLOCK : (block + 1) * VBLOCK
                    ]

    width = GROUP * VBLOCK
    distance = (
        lax.rem(lax.broadcasted_iota(jnp.int32, (window, width), 1), VBLOCK)
        - lax.broadcasted_iota(jnp.int32, (window, width), 0)
        + MARGIN
    ).astype(F32)

    def warp_columns(group):
        for camera in range(cameras):
            rows = bands[camera, group]
            tap_of = distance - rows[TAPS : TAPS + 1]
            matrix = jnp.zeros((window, width), F32)
            for tap in range(TAPS):
                matrix = jnp.where(tap_of == float(tap), rows[tap : tap + 1], matrix)
            matrix = matrix.astype(BF16)
            for block in range(blocks):
                place = slice(block * VBLOCK, block * VBLOCK + window)
                total[camera, place] = total[camera, place] + jnp.dot(
                    matrix, mixed[camera, block], preferred_element_type=F32
                )

    @pl.when(step == 0)
    def _():
        total[...] = jnp.zeros_like(total)
        volume[...] = jnp.zeros_like(volume)
        gate_second(sphere_rim[0], 0, 0, 2)
        gate_second(sphere_rim[1], 1, 1, 3)
        gate_second(masked(cot_zero[0], second_zero[0]), 2, 2, 0)
        gate_second(masked(cot_zero[1], second_zero[1]), 3, 3, 1)
        order = (2, 3, 0, 1)
        for index in range(2):
            hidden = jnp.zeros((wide, merged), F32)
            for depth in range(3):
                hidden = hidden + jnp.dot(
                    taps_one[order[index + 2 - depth]],
                    mixer_second[depth],
                    preferred_element_type=F32,
                )
            saved = sphere_rim[2] if index == 0 else first_zero[0]
            gate_first(hidden, saved, index, index + 1, index)

    base = step * GROUP
    before = jnp.maximum(step - 1, 0)

    gate_second(masked(cot_a[0], second_a[0]), 0, base + 4, 2)
    gate_second(masked(cot_a[1], second_a[1]), 1, base + 5, 3)
    hidden = conv(taps_one, mixer_second, (0, 1))
    gate_first(hidden[:wide], first_a[0], 0, base + 3, 2)
    gate_first(hidden[wide:], first_b[0], 1, base + 4, 3)
    for index in range(2):
        grad = masked(cot_b[index], second_b[index])
        grad = jnp.where(last, sphere_rim[3 + index], grad)
        gate_second(grad, 2 + index, base + 6 + index, 4 + index)
    mix_rows(before)
    hidden = conv(taps_one, mixer_second, (2, 3))
    gate_first(hidden[:wide], first_c[0], 2, base + 5, 4)
    gate_first(
        hidden[wide:], jnp.where(last, sphere_rim[5], first_d[0]), 3, base + 6, 5
    )
    for pair in range(2):
        value = conv(taps_two, mixer_first, (2 * pair, 2 * pair + 1)).astype(BF16)
        volume[2 * pair] = value[:columns]
        volume[2 * pair + 1] = value[columns:]
        if pair == 0:
            warp_columns(before)
    for slot in range(2):
        taps_one[slot] = taps_one[slot + 4]
        taps_two[slot] = taps_two[slot + 4]

    @pl.when(last)
    def _():
        mix_rows(step)
        warp_columns(step)
        for row in range(row_count):
            out_ref[row] = jnp.concatenate(
                [
                    total[camera, :, row * channels : (row + 1) * channels]
                    for camera in range(cameras)
                ],
                axis=1,
            )


def sweep(sphere_rim, column_rim, cot, second, first, mixer_second, mixer_first, resample, bands):
    spheres, columns, merged = cot.shape
    cameras, row_count = resample.shape[1:3]
    channels = merged // row_count
    wide = columns + 16
    blocks = columns // VBLOCK
    window = VBLOCK + 2 * MARGIN
    pairs = spheres // 2

    def whole(array):
        zeros = (0,) * array.ndim
        return pl.BlockSpec(
            array.shape, lambda g: zeros, pipeline_mode=pl.Buffered(buffer_count=1)
        )

    pair_a = pl.BlockSpec((2, columns, merged), lambda g: (2 * g + 1, 0, 0))
    pair_b = pl.BlockSpec(
        (2, columns, merged), lambda g: (jnp.minimum(2 * g + 2, pairs - 1), 0, 0)
    )
    pair_zero = pl.BlockSpec(
        (2, columns, merged), lambda g: (0, 0, 0), pipeline_mode=pl.Buffered(buffer_count=1)
    )
    single = lambda ahead: pl.BlockSpec(
        (1, columns, merged),
        lambda g: (jnp.minimum(GROUP * g + ahead, spheres - 1), 0, 0),
    )
    single_zero = pl.BlockSpec(
        (1, columns, merged), lambda g: (0, 0, 0), pipeline_mode=pl.Buffered(buffer_count=1)
    )
    extended = columns + 2 * MARGIN
    out_shape = (row_count, extended, cameras * channels)
    flops = 2 * spheres * columns * merged * merged * (18 + cameras + cameras // 2)
    return pl.pallas_call(
        sweep_kernel,
        grid=(spheres // GROUP,),
        in_specs=[
            whole(sphere_rim),
            whole(column_rim),
            pair_a,
            pair_b,
            pair_zero,
            pair_a,
            pair_b,
            pair_zero,
            single(1),
            single(2),
            single(3),
            single(4),
            single_zero,
            whole(mixer_second),
            whole(mixer_first),
            whole(resample),
            whole(bands),
        ],
        out_specs=pl.BlockSpec(
            out_shape, lambda g: (0, 0, 0), pipeline_mode=pl.Buffered(buffer_count=1)
        ),
        out_shape=jax.ShapeDtypeStruct(out_shape, F32),
        scratch_shapes=[
            pltpu.VMEM((6, wide, 3 * merged), BF16),
            pltpu.VMEM((6, columns, 3 * merged), BF16),
            pltpu.VMEM((4, columns + 32, merged), F32),
            pltpu.VMEM((4, wide, merged), F32),
            pltpu.VMEM((GROUP, columns, merged), BF16),
            pltpu.VMEM((cameras, blocks, GROUP * VBLOCK, merged), BF16),
            pltpu.VMEM((cameras, extended, merged), F32),
        ],
        compiler_params=pltpu.CompilerParams(
            dimension_semantics=("arbitrary",), vmem_limit_bytes=56 * 2**20
        ),
        cost_estimate=pl.CostEstimate(
            flops=flops, bytes_accessed=3 * cot.size * 2, transcendentals=0
        ),
        name="sweep",
    )(
        sphere_rim,
        column_rim,
        cot,
        cot,
        cot,
        second,
        second,
        second,
        first,
        first,
        first,
        first,
        first,
        mixer_second,
        mixer_first,
        resample,
        bands,
    )


def row_mixers(kernel, row_count):
    channels = kernel.shape[3]
    strip = jnp.transpose(kernel, (0, 1, 4, 2, 3)).reshape(9, channels, 3 * channels)
    merged = row_count * channels
    strip = jnp.pad(strip, ((0, 0), (0, 0), (merged, merged)))
    rows = [
        lax.slice_in_dim(
            strip, merged - (row - 1) * channels, 2 * merged - (row - 1) * channels, axis=2
        )
        for row in range(row_count)
    ]
    return jnp.stack(rows, axis=1).reshape(3, 3 * merged, merged)


def steps_along(axis, offset):
    count = lax.axis_size(axis)
    return [(i, i + offset) for i in range(count) if 0 <= i + offset < count]


def ring_along(axis, offset):
    count = lax.axis_size(axis)
    return [(i, (i + offset) % count) for i in range(count)]


def joint(depth_pairs, azim_pairs):
    width = lax.axis_size("azim")
    return [
        (d0 * width + a0, d1 * width + a1)
        for d0, d1 in depth_pairs
        for a0, a1 in azim_pairs
    ]


def body(cot, second, first, kernel_first, kernel_second, row_resample, col_taps, band_width, col_offset):
    spheres, columns, merged = cot.shape
    cameras, _, row_count, _ = row_resample.shape
    channels = merged // row_count
    gate = lambda where: jnp.where(second[where] > 0, cot[where], jnp.zeros((), BF16))
    everything = slice(None)

    def edge(sphere_slice, column_slice, sphere_first, column_first, axis):
        return jnp.concatenate(
            [gate((sphere_slice, column_slice)), first[sphere_first, column_first]], axis=axis
        )

    left = edge(everything, slice(0, 2), everything, slice(0, 1), 1)
    right = edge(everything, slice(columns - 2, None), everything, slice(columns - 1, None), 1)
    low = edge(slice(0, 2), everything, slice(0, 1), everything, 0)
    high = edge(slice(spheres - 2, None), everything, slice(spheres - 1, None), everything, 0)
    forward, backward = ring_along("azim", 1), ring_along("azim", -1)
    up, down = steps_along("depth", 1), steps_along("depth", -1)
    both = ("depth", "azim")
    from_left = lax.ppermute(right, "azim", forward)
    from_right = lax.ppermute(left, "azim", backward)
    from_low = lax.ppermute(high, "depth", up)
    from_high = lax.ppermute(low, "depth", down)

    def corner(side):
        return jnp.concatenate([side[:2], side[spheres - 2 :]], axis=0)

    corners = {}
    for name, source, azim_pairs in (("left", right, forward), ("right", left, backward)):
        below = lax.ppermute(source[spheres - 2 :], both, joint(up, azim_pairs))
        above = lax.ppermute(source[:2], both, joint(down, azim_pairs))
        corners[name] = (below, above)
    side_left = jnp.concatenate([corners["left"][0], from_left, corners["left"][1]], axis=0)
    side_right = jnp.concatenate([corners["right"][0], from_right, corners["right"][1]], axis=0)
    blank = lambda rows: jnp.zeros((spheres + 4, rows, merged), BF16)
    column_rim = jnp.concatenate(
        [
            blank(6),
            side_left[:, :2],
            side_right[:, :2],
            blank(6),
            blank(7),
            side_left[:, 2:],
            side_right[:, 2:],
            blank(7),
        ],
        axis=1,
    )
    sphere_rim = jnp.concatenate([from_low, from_high], axis=0)

    mixer_second = row_mixers(kernel_second, row_count)
    mixer_first = row_mixers(kernel_first, row_count)
    resample = jnp.repeat(jnp.transpose(row_resample, (1, 0, 2, 3)), channels, axis=3)
    keep = lax.broadcasted_iota(jnp.int32, col_taps.shape, 2) < band_width[:, :, None]
    taps = jnp.where(keep, col_taps, 0.0).astype(BF16).astype(F32)
    table = jnp.concatenate([taps, col_offset[:, :, None].astype(F32)], axis=2)
    table = jnp.transpose(
        table.reshape(cameras, spheres // GROUP, GROUP, TAPS + 1), (0, 1, 3, 2)
    )
    table = jnp.repeat(table, VBLOCK, axis=3)
    bands = jnp.pad(table, ((0, 0), (0, 0), (0, 7), (0, 0)))

    partial = sweep(
        sphere_rim, column_rim, cot, second, first, mixer_second, mixer_first, resample, bands
    )

    spill_left = lax.ppermute(partial[:, :MARGIN], "azim", backward)
    spill_right = lax.ppermute(partial[:, columns + MARGIN :], "azim", forward)
    inner = partial[:, MARGIN : columns + MARGIN]
    inner = inner.at[:, columns - MARGIN :].add(spill_left)
    inner = inner.at[:, :MARGIN].add(spill_right)
    return lax.psum_scatter(inner, "depth", scatter_dimension=0, tiled=True)


def solution(mesh):
    placed = (
        P("depth", "azim", None),
        P("depth", "azim", None),
        P("depth", "azim", None),
        P(),
        P(),
        P(None, "depth", None, None),
        P(None, "depth", None),
        P(None, "depth"),
        P(None, "depth"),
    )
    return jax.shard_map(
        body, mesh=mesh, in_specs=placed, out_specs=P("depth", "azim", None), check_vma=False
    )
```

```python
import functools

import jax
import jax.numpy as jnp
from jax import lax
from jax.experimental import pallas as pl
from jax.experimental.pallas import tpu as pltpu
from jax.sharding import PartitionSpec as P

TAPS = 8
SHIFT = 24
MARGIN = SHIFT + TAPS
GROUP = 4
VBLOCK = 64
SLOT = 16
BF16 = jnp.bfloat16
F32 = jnp.float32


def edge_kernel(
    side, cot_left, cot_right, second_left, second_right, first_left, first_right,
    cot_rim, second_rim, first_rim, left, right, rim, corner_left, corner_right,
):
    spheres = cot_left.shape[0]
    gate = lambda cot, saved: jnp.where(saved > 0, cot, jnp.zeros_like(cot))
    top = side[0]
    for message, corner, cot, saved, kept, columns, one in (
        (left, corner_left, cot_left, second_left, first_left, slice(0, 2), slice(0, 1)),
        (right, corner_right, cot_right, second_right, first_right, slice(6, 8), slice(7, 8)),
    ):
        message[:, 0:2] = gate(cot[:, columns], saved[:, columns])
        message[:, 2:3] = kept[:, one]
        message[:, 3:4] = kept[:, one]
        for index in range(2):
            sphere = top * (spheres - 1) + (1 - 2 * top) * index
            corner[index, 0:2] = gate(cot[sphere, columns], saved[sphere, columns])
            corner[index, 2:3] = kept[sphere, one]
            corner[index, 3:4] = kept[sphere, one]
    for index in range(2):
        place = top + (1 - 2 * top) * index
        rim[index] = gate(cot_rim[place], second_rim[place])
    rim[2] = first_rim[0]


def edges(side, cot, second, first):
    spheres, columns, merged = cot.shape
    pairs = spheres // 2
    low = pl.BlockSpec((spheres, 8, merged), lambda g, s: (0, 0, 0))
    high = pl.BlockSpec((spheres, 8, merged), lambda g, s: (0, columns // 8 - 1, 0))
    pair = pl.BlockSpec((2, columns, merged), lambda g, s: (s[0] * (pairs - 1), 0, 0))
    one = pl.BlockSpec((1, columns, merged), lambda g, s: (s[0] * (spheres - 1), 0, 0))
    shapes = (
        (spheres, 4, merged), (spheres, 4, merged), (3, columns, merged),
        (2, 4, merged), (2, 4, merged),
    )
    return pl.pallas_call(
        edge_kernel,
        grid_spec=pltpu.PrefetchScalarGridSpec(
            num_scalar_prefetch=1,
            grid=(1,),
            in_specs=[low, high, low, high, low, high, pair, pair, one],
            out_specs=[pl.BlockSpec(s, lambda g, s: (0, 0, 0)) for s in shapes],
        ),
        out_shape=[jax.ShapeDtypeStruct(s, BF16) for s in shapes],
        name="edges",
    )(side, cot, cot, second, second, first, first, cot, second, first)


def sweep_kernel(names, first_group, head, tail, row_count, pair_rows, *refs):
    ref = dict(zip(names, refs))
    flip = ref["info"][0]
    step = pl.program_id(0)
    group = step + first_group
    from_left, from_right = ref["from_left"], ref["from_right"]
    spheres, _, merged = from_left.shape
    taps_one, taps_two = ref["taps_one"], ref["taps_two"]
    columns = taps_two.shape[1]
    volume, mixed, total = ref["volume"], ref["mixed"], ref["total"]
    cameras = total.shape[0]
    channels = merged // row_count
    wide = columns + 16
    blocks = columns // VBLOCK
    window = VBLOCK + 2 * MARGIN
    padded_one, padded_two = ref["padded_one"], ref["padded_two"]
    actual = lambda v: flip * (spheres - 1) + (1 - 2 * flip) * v
    inner = lambda i: flip + (1 - 2 * flip) * i
    mixer_at = lambda name, depth: ref[name][2 * flip + (1 - 2 * flip) * depth]

    def store_taps(source, target, slot, rows):
        for tap in range(3):
            target[slot, :, tap * merged : (tap + 1) * merged] = source[
                9 - tap : 9 - tap + rows
            ].astype(BF16)

    def gate_second(grad, sides, index, slot):
        padded = padded_one.at[index]
        padded[16 : 16 + columns] = grad.astype(F32)
        padded[14:16] = sides[0][0:2].astype(F32)
        padded[16 + columns : 18 + columns] = sides[1][0:2].astype(F32)
        store_taps(padded, taps_one, slot, wide)

    def masked(cot, saved):
        return jnp.where(saved > 0, cot, jnp.zeros_like(cot))

    def sides_of(v):
        sphere = actual(v)
        return from_left[sphere], from_right[sphere]

    def old(name, slot):
        if tail and slot < 2:
            return ref["carry_" + name][slot]
        return ref[name][slot]

    def conv(name, mixers, slots):
        lhs = lambda depth: jnp.concatenate(
            [old(name, slot + 2 - depth) for slot in slots], axis=0
        )
        value = jnp.dot(lhs(2), mixer_at(mixers, 2), preferred_element_type=F32)
        value = value + jnp.dot(lhs(1), mixer_at(mixers, 1), preferred_element_type=F32)
        return value + jnp.dot(lhs(0), mixer_at(mixers, 0), preferred_element_type=F32)

    def gate_first(hidden, saved, sides, index, slot):
        low = jnp.broadcast_to(sides[0][2:3].astype(F32), (8, merged))
        high = jnp.broadcast_to(sides[1][2:3].astype(F32), (8, merged))
        keep = jnp.concatenate([low, saved.astype(F32), high], axis=0) > 0
        padded_two[index] = jnp.where(keep, hidden, 0.0)
        store_taps(padded_two.at[index], taps_two, slot, columns)

    lane = lax.broadcasted_iota(jnp.int32, (channels, merged), 1)
    sub = lax.broadcasted_iota(jnp.int32, (channels, merged), 0)
    diagonal = lax.rem(lane, channels) == sub
    table_lanes = cameras * row_count * row_count
    owner = lax.broadcasted_iota(
        jnp.int32, (cameras * row_count, table_lanes), 1
    ) // row_count == lax.broadcasted_iota(jnp.int32, (cameras * row_count, table_lanes), 0)

    def mix_rows(group, source):
        rows = [
            jnp.where(owner, ref["row_table"][actual(group * GROUP + sphere)], 0.0)
            for sphere in range(GROUP)
        ]
        spread = jnp.dot(
            jnp.concatenate(rows, axis=0).astype(BF16),
            ref["expand"][...],
            preferred_element_type=F32,
        )
        for camera in range(cameras):
            for sphere in range(GROUP):
                start = (sphere * cameras + camera) * row_count
                weights = jnp.concatenate(
                    [
                        jnp.where(diagonal, spread[start + r : start + r + 1], 0.0)
                        for r in range(row_count)
                    ],
                    axis=0,
                ).astype(BF16)
                value = jnp.dot(
                    source[sphere], weights, preferred_element_type=F32
                ).astype(BF16)
                for block in range(blocks):
                    mixed[camera, block, sphere * VBLOCK : (sphere + 1) * VBLOCK] = value[
                        block * VBLOCK : (block + 1) * VBLOCK
                    ]

    width = GROUP * VBLOCK
    distance = (
        lax.rem(lax.broadcasted_iota(jnp.int32, (window, width), 1), VBLOCK)
        - lax.broadcasted_iota(jnp.int32, (window, width), 0)
        + MARGIN
    ).astype(F32)

    def warp_columns(group):
        quarter = lax.broadcasted_iota(jnp.int32, (spheres, width), 1) // VBLOCK
        chosen = lax.broadcasted_iota(jnp.int32, (spheres, width), 0) == actual(
            group * GROUP + quarter
        )
        rows_all = jnp.dot(
            ref["tap_table"][...], chosen.astype(BF16), preferred_element_type=F32
        )
        for camera in range(cameras):
            rows = rows_all[camera * SLOT : (camera + 1) * SLOT]
            tap_of = distance - rows[TAPS : TAPS + 1]
            matrix = jnp.zeros((window, width), F32)
            for tap in range(TAPS):
                matrix = jnp.where(tap_of == float(tap), rows[tap : tap + 1], matrix)
            matrix = matrix.astype(BF16)
            for block in range(blocks):
                place = slice(block * VBLOCK, block * VBLOCK + window)
                total[camera, place] = total[camera, place] + jnp.dot(
                    matrix, mixed[camera, block], preferred_element_type=F32
                )

    @pl.when(step == 0)
    def _():
        from_table = lax.broadcasted_iota(jnp.int32, (table_lanes, merged), 0)
        to_lane = lax.broadcasted_iota(jnp.int32, (table_lanes, merged), 1)
        ref["expand"][...] = jnp.where(
            lax.rem(from_table, row_count) == to_lane // channels, 1.0, 0.0
        ).astype(BF16)
        if not head:
            total[...] = ref["carry_total"][...]
            return
        total[...] = jnp.zeros_like(total)
        volume[...] = jnp.zeros_like(volume)
        if "low_rim" in ref:
            low_rim = ref["low_rim"]
            for index in range(2):
                sides = ref["low_left"][1 - index], ref["low_right"][1 - index]
                gate_second(low_rim[1 - index], sides, index, 2 + index)
        else:
            taps_one[2] = jnp.zeros_like(taps_one[2])
            taps_one[3] = jnp.zeros_like(taps_one[3])
        for index in range(2):
            place = inner(index)
            grad = masked(ref["cot_zero"][place], ref["second_zero"][place])
            gate_second(grad, sides_of(index), 2 + index, index)
        order = (2, 3, 0, 1)
        for index in range(2):
            if index == 0 and "low_rim" not in ref:
                taps_two[0] = jnp.zeros_like(taps_two[0])
                continue
            hidden = jnp.zeros((wide, merged), F32)
            for depth in range(3):
                hidden = hidden + jnp.dot(
                    taps_one[order[index + 2 - depth]],
                    mixer_at("mixer_second", depth),
                    preferred_element_type=F32,
                )
            if index == 0:
                saved = ref["low_rim"][2]
                sides = ref["low_left"][0], ref["low_right"][0]
            else:
                saved = ref["first_zero"][0]
                sides = sides_of(0)
            gate_first(hidden, saved, sides, index, index)

    base = group * GROUP
    before = jnp.maximum(group - 1, 0)

    for index in range(2):
        place = inner(index)
        grad = masked(ref["cot_a"][place], ref["second_a"][place])
        gate_second(grad, sides_of(base + 2 + index), index, 2 + index)
    hidden = conv("taps_one", "mixer_second", (0, 1))
    gate_first(hidden[:wide], ref["first_a"][0], sides_of(base + 1), 0, 2)
    gate_first(hidden[wide:], ref["first_b"][0], sides_of(base + 2), 1, 3)
    for index in range(2):
        if tail:
            grad = ref["high_rim"][index]
            sides = ref["high_left"][index], ref["high_right"][index]
        else:
            place = inner(index)
            grad = masked(ref["cot_b"][place], ref["second_b"][place])
            sides = sides_of(base + 4 + index)
        gate_second(grad, sides, 2 + index, 4 + index)
    mix_rows(before, ref["carry_volume"] if tail else volume)
    hidden = conv("taps_one", "mixer_second", (2, 3))
    gate_first(hidden[:wide], ref["first_c"][0], sides_of(base + 3), 2, 4)
    if tail:
        saved = ref["high_rim"][2]
        sides = ref["high_left"][0], ref["high_right"][0]
    else:
        saved = ref["first_d"][0]
        sides = sides_of(base + 4)
    gate_first(hidden[wide:], saved, sides, 3, 5)
    for pair in range(2):
        value = conv("taps_two", "mixer_first", (2 * pair, 2 * pair + 1)).astype(BF16)
        volume[2 * pair] = value[:columns]
        volume[2 * pair + 1] = value[columns:]
        if pair == 0:
            warp_columns(before)

    if not tail:
        for slot in range(2):
            taps_one[slot] = taps_one[slot + 4]
            taps_two[slot] = taps_two[slot + 4]

        @pl.when(step == pl.num_programs(0) - 1)
        def _():
            for slot in range(2):
                ref["next_taps_one"][slot] = taps_one[slot]
                ref["next_taps_two"][slot] = taps_two[slot]
            ref["next_volume"][...] = volume[...]
            ref["next_total"][...] = total[...]

        return

    mix_rows(group, volume)
    warp_columns(group)

    def joined(row, place):
        return jnp.concatenate(
            [
                total[camera, place, row * channels : (row + 1) * channels]
                for camera in range(cameras)
            ],
            axis=1,
        )

    everything = slice(0, columns + 2 * MARGIN)
    if not pair_rows:
        for row in range(row_count):
            ref["whole"][row] = joined(row, everything)
        return
    half = row_count // 2
    own_high = ref["info"][1] > 0
    for row in range(half):
        low, high = joined(row, everything), joined(row + half, everything)
        for prefix, value in (
            ("own", jnp.where(own_high, high, low)),
            ("peer", jnp.where(own_high, low, high)),
        ):
            main = value[MARGIN : MARGIN + columns]
            ref[prefix][row] = main if prefix == "own" else main.astype(BF16)
            ref[prefix + "_left"][row] = value[:MARGIN].astype(BF16)
            ref[prefix + "_right"][row] = value[MARGIN + columns :].astype(BF16)


def sweep(first_group, count, head, tail, info, arrays, carry, row_count, pair_rows):
    cot, second, first = arrays["cot"], arrays["second"], arrays["first"]
    spheres, columns, merged = cot.shape
    cameras = arrays["cameras"]
    wide = columns + 16
    extended = columns + 2 * MARGIN
    pairs = spheres // 2
    channels = merged // row_count
    names, specs, operands = [], [], []

    def add(name, array, spec):
        names.append(name)
        specs.append(spec)
        operands.append(array)

    def whole(shape):
        zeros = (0,) * len(shape)
        return pl.BlockSpec(
            shape, lambda g, s: zeros, pipeline_mode=pl.Buffered(buffer_count=1)
        )

    def spheres_at(size, place, **more):
        limit = spheres // size - 1
        return pl.BlockSpec(
            (size, columns, merged),
            lambda g, s: (s[0] * limit + (1 - 2 * s[0]) * place(g + first_group), 0, 0),
            **more,
        )

    for name in ("from_left", "from_right", "mixer_second", "mixer_first", "row_table", "tap_table"):
        add(name, arrays[name], whole(arrays[name].shape))
    rims = (("low_rim", "low_left", "low_right") if head else ()) + (
        ("high_rim", "high_left", "high_right") if tail else ()
    )
    for name in rims:
        if name in arrays:
            add(name, arrays[name], whole(arrays[name].shape))
    for name, array in (("cot", cot), ("second", second)):
        add(name + "_a", array, spheres_at(2, lambda g: 2 * g + 1))
        if not tail:
            add(name + "_b", array, spheres_at(2, lambda g: 2 * g + 2))
        if head:
            add(name + "_zero", array, spheres_at(2, lambda g: 0, pipeline_mode=pl.Buffered(buffer_count=1)))
    for ahead, letter in ((1, "a"), (2, "b"), (3, "c"), (4, "d")):
        if not (tail and ahead == 4):
            add("first_" + letter, first, spheres_at(1, lambda g, ahead=ahead: GROUP * g + ahead))
    if head:
        add("first_zero", first, spheres_at(1, lambda g: 0, pipeline_mode=pl.Buffered(buffer_count=1)))
    carried = {
        "taps_one": ((2, wide, 3 * merged), BF16),
        "taps_two": ((2, columns, 3 * merged), BF16),
        "volume": ((GROUP, columns, merged), BF16),
        "total": ((cameras, extended, merged), F32),
    }
    if not head:
        for name in carried:
            add("carry_" + name, carry[name], whole(carried[name][0]))
    outputs = {}
    if not tail:
        outputs = {"next_" + name: value for name, value in carried.items()}
    elif pair_rows:
        half, lanes = row_count // 2, cameras * channels
        for prefix in ("own", "peer"):
            outputs[prefix] = ((half, columns, lanes), F32 if prefix == "own" else BF16)
            outputs[prefix + "_left"] = ((half, MARGIN, lanes), BF16)
            outputs[prefix + "_right"] = ((half, MARGIN, lanes), BF16)
    else:
        outputs["whole"] = ((row_count, extended, cameras * channels), F32)
    scratch = {
        "taps_one": ((6, wide, 3 * merged), BF16),
        "taps_two": ((6, columns, 3 * merged), BF16),
        "padded_one": ((4, columns + 32, merged), F32),
        "padded_two": ((4, wide, merged), F32),
        "volume": carried["volume"],
        "mixed": ((cameras, columns // VBLOCK, GROUP * VBLOCK, merged), BF16),
        "total": carried["total"],
        "expand": ((cameras * row_count * row_count, merged), BF16),
    }
    every = ["info", *names, *outputs, *scratch]
    flops = 2 * GROUP * count * columns * merged * merged * (18 + cameras + cameras // 2)
    results = pl.pallas_call(
        functools.partial(
            sweep_kernel, every, first_group, head, tail, row_count, pair_rows
        ),
        grid_spec=pltpu.PrefetchScalarGridSpec(
            num_scalar_prefetch=1,
            grid=(count,),
            in_specs=specs,
            out_specs=[whole(shape) for shape, _ in outputs.values()],
            scratch_shapes=[pltpu.VMEM(shape, kind) for shape, kind in scratch.values()],
        ),
        out_shape=[jax.ShapeDtypeStruct(shape, kind) for shape, kind in outputs.values()],
        compiler_params=pltpu.CompilerParams(
            dimension_semantics=("arbitrary",), vmem_limit_bytes=56 * 2**20
        ),
        cost_estimate=pl.CostEstimate(
            flops=flops, bytes_accessed=3 * GROUP * count * columns * merged * 2, transcendentals=0
        ),
        name="sweep_tail" if tail else "sweep",
    )(info, *operands)
    return {name.removeprefix("next_"): result for name, result in zip(outputs, results)}


def finish_kernel(own, peer, own_left, own_right, peer_left, peer_right, out):
    columns = out.shape[1]
    out[...] = own[...] + peer[...].astype(F32)
    start, end = slice(0, MARGIN), slice(columns - MARGIN, columns)
    out[:, start] = out[:, start] + (own_left[...].astype(F32) + peer_left[...].astype(F32))
    out[:, end] = out[:, end] + (own_right[...].astype(F32) + peer_right[...].astype(F32))


def row_mixers(kernel, row_count):
    channels = kernel.shape[3]
    strip = jnp.transpose(kernel, (0, 1, 4, 2, 3)).reshape(9, channels, 3 * channels)
    merged = row_count * channels
    strip = jnp.pad(strip, ((0, 0), (0, 0), (merged, merged)))
    rows = [
        lax.slice_in_dim(
            strip, merged - (row - 1) * channels, 2 * merged - (row - 1) * channels, axis=2
        )
        for row in range(row_count)
    ]
    return jnp.stack(rows, axis=1).reshape(3, 3 * merged, merged)


def ring(offset):
    count = lax.axis_size("azim")
    return [(i, (i + offset) % count) for i in range(count)]


def stride(offset):
    count = lax.axis_size("depth")
    if count == 2:
        return [(0, 1), (1, 0)]
    return [(i, i + offset) for i in range(count) if 0 <= i + offset < count]


def joint(depth_pairs, azim_pairs):
    width = lax.axis_size("azim")
    return [
        (d0 * width + a0, d1 * width + a1)
        for d0, d1 in depth_pairs
        for a0, a1 in azim_pairs
    ]


def body(cot, second, first, kernel_first, kernel_second, row_resample, col_taps, band_width, col_offset):
    spheres, columns, merged = cot.shape
    cameras, _, row_count, _ = row_resample.shape
    depth_index = lax.axis_index("depth").astype(jnp.int32)
    paired = lax.axis_size("depth") == 2
    both = ("depth", "azim")
    forward, backward = ring(1), ring(-1)
    arrays = {"cot": cot, "second": second, "first": first, "cameras": cameras}

    def send_rims(prefix, offset, side):
        left, right, rim, corner_left, corner_right = edges(
            jnp.full((1,), side, jnp.int32), cot, second, first
        )
        if "from_left" not in arrays:
            arrays["from_left"] = lax.ppermute(right, "azim", forward)
            arrays["from_right"] = lax.ppermute(left, "azim", backward)
        pairs = stride(offset)
        arrays[prefix + "_rim"] = lax.ppermute(rim, "depth", pairs)
        arrays[prefix + "_left"] = lax.ppermute(corner_right, both, joint(pairs, forward))
        arrays[prefix + "_right"] = lax.ppermute(corner_left, both, joint(pairs, backward))

    if paired:
        send_rims("high", -1, 1 - depth_index)
        flip = depth_index
    else:
        send_rims("low", 1, 1)
        send_rims("high", -1, 0)
        flip = jnp.zeros((), jnp.int32)
    info = jnp.stack([flip, depth_index])

    arrays["mixer_second"] = row_mixers(kernel_second, row_count)
    arrays["mixer_first"] = row_mixers(kernel_first, row_count)
    arrays["row_table"] = jnp.transpose(row_resample, (1, 0, 2, 3)).reshape(spheres, 1, -1)
    keep = lax.broadcasted_iota(jnp.int32, col_taps.shape, 2) < band_width[:, :, None]
    taps = jnp.where(keep, col_taps, 0.0)
    table = jnp.concatenate([taps, col_offset[:, :, None].astype(F32)], axis=2)
    table = jnp.pad(jnp.transpose(table, (0, 2, 1)), ((0, 0), (0, SLOT - TAPS - 1), (0, 0)))
    arrays["tap_table"] = table.reshape(cameras * SLOT, spheres).astype(BF16)

    groups = spheres // GROUP
    carry = sweep(0, groups - 1, True, False, info, arrays, None, row_count, paired)
    parts = sweep(groups - 1, 1, False, True, info, arrays, carry, row_count, paired)

    if paired:
        swap = [(0, 1), (1, 0)]
        got = (
            lax.ppermute(parts["peer"], "depth", swap),
            lax.ppermute(parts["own_right"], "azim", forward),
            lax.ppermute(parts["own_left"], "azim", backward),
            lax.ppermute(parts["peer_right"], both, joint(swap, forward)),
            lax.ppermute(parts["peer_left"], both, joint(swap, backward)),
        )
        return pl.pallas_call(
            finish_kernel,
            out_shape=jax.ShapeDtypeStruct(parts["own"].shape, F32),
            name="finish",
        )(parts["own"], *got)
    partial = parts["whole"]
    spill_left = lax.ppermute(partial[:, :MARGIN], "azim", backward)
    spill_right = lax.ppermute(partial[:, columns + MARGIN :], "azim", forward)
    inner = partial[:, MARGIN : columns + MARGIN]
    inner = inner.at[:, columns - MARGIN :].add(spill_left)
    inner = inner.at[:, :MARGIN].add(spill_right)
    return lax.psum_scatter(inner, "depth", scatter_dimension=0, tiled=True)


def solution(mesh):
    placed = (
        P("depth", "azim", None),
        P("depth", "azim", None),
        P("depth", "azim", None),
        P(),
        P(),
        P(None, "depth", None, None),
        P(None, "depth", None),
        P(None, "depth"),
        P(None, "depth"),
    )
    return jax.shard_map(
        body, mesh=mesh, in_specs=placed, out_specs=P("depth", "azim", None), check_vma=False
    )
```

```python
import functools
from types import SimpleNamespace

import jax
import jax.numpy as jnp
from jax import lax
from jax.experimental import pallas as pl
from jax.experimental.pallas import tpu as pltpu
from jax.sharding import PartitionSpec as P

TAPS = 8
SHIFT = 24
HALO = 4
LEAD = 2
LEFT = 40
RIGHT = 24
GROUP = 4
VBLOCK = 64
WINDOW = VBLOCK + LEFT + RIGHT
SLOT = 16
UNROLL = 1
BF16 = jnp.bfloat16
F32 = jnp.float32


def edge_kernel(
    side, cot_right, second_right, first_right, cot_rim, second_rim, first_rim, right, rim, corner
):
    spheres = cot_right.shape[0]
    gate = lambda cot, saved: jnp.where(saved > 0, cot, jnp.zeros_like(cot))
    top = side[0]
    for index in range(2):
        place = top + (1 - 2 * top) * index
        rim[index] = gate(cot_rim[place], second_rim[place])
    rim[2] = first_rim[0]
    last = slice(8 - HALO, 8)
    right[:, 0:HALO] = gate(cot_right[:, last], second_right[:, last])
    right[:, HALO : 2 * HALO] = first_right[:, last]
    for index in range(2):
        corner[index] = right[top * (spheres - 1) + (1 - 2 * top) * index]


def edges(side, cot, second, first):
    spheres, columns, merged = cot.shape
    pairs = spheres // 2
    high = pl.BlockSpec((spheres, 8, merged), lambda g, s: (0, columns // 8 - 1, 0))
    pair = pl.BlockSpec((2, columns, merged), lambda g, s: (s[0] * (pairs - 1), 0, 0))
    one = pl.BlockSpec((1, columns, merged), lambda g, s: (s[0] * (spheres - 1), 0, 0))
    shapes = ((spheres, 2 * HALO, merged), (3, columns, merged), (2, 2 * HALO, merged))
    return pl.pallas_call(
        edge_kernel,
        grid_spec=pltpu.PrefetchScalarGridSpec(
            num_scalar_prefetch=1,
            grid=(1,),
            in_specs=[high, high, high, pair, pair, one],
            out_specs=[pl.BlockSpec(s, lambda g, s: (0, 0, 0)) for s in shapes],
        ),
        out_shape=[jax.ShapeDtypeStruct(s, BF16) for s in shapes],
        name="edges",
    )(side, cot, second, first, cot, second, first)


def block_start(flip, sphere, count, spheres):
    sphere = jnp.minimum(sphere, spheres - count)
    return sphere + flip * (spheres - count - 2 * sphere)


def sweep_kernel(names, row_count, paired, *refs):
    ref = SimpleNamespace(**dict(zip(names, refs)))
    flip = ref.info[0]
    step = pl.program_id(0)
    last = step == pl.num_programs(0) - 1
    spheres, _, merged = ref.from_left.shape
    taps_one, taps_two = ref.taps_one, ref.taps_two
    columns = taps_two.shape[1]
    volume, mixed, total = ref.volume, ref.mixed, ref.total
    cameras = total.shape[0]
    channels = merged // row_count
    wide = columns + 16
    blocks = columns // VBLOCK
    actual = lambda v: flip * (spheres - 1) + (1 - 2 * flip) * v
    inner = lambda i: flip + (1 - 2 * flip) * i
    mixer_at = lambda mixers, depth: mixers[depth]

    def store_taps(source, target, slot, first_row, rows):
        for tap in range(3):
            target[slot, :, tap * merged : (tap + 1) * merged] = source[
                first_row - tap : first_row - tap + rows
            ].astype(BF16)

    def gate_second(grad, side, index, slot):
        padded = ref.padded_one.at[index]
        padded[16 : 16 + columns] = grad.astype(F32)
        padded[16 - HALO : 16] = side[0:HALO].astype(F32)
        store_taps(padded, taps_one, slot, 9, wide)

    def masked(cot, saved):
        return jnp.where(saved > 0, cot, jnp.zeros_like(cot))

    def gated(v, first_sphere):
        place = inside(v, first_sphere, ref.cot.shape[0])
        return masked(ref.cot[place], ref.second[place])

    def inside(v, first_sphere, count):
        start = block_start(flip, first_sphere, count, spheres)
        return actual(jnp.minimum(v, spheres - 1)) - start

    def side_of(v):
        return ref.from_left[actual(jnp.minimum(v, spheres - 1))]

    def conv(source, mixers, slot):
        value = None
        for depth in (2, 1, 0):
            lhs = jnp.concatenate(
                [source[slot + 2 - depth], source[slot + 3 - depth]], axis=0
            )
            part = jnp.dot(lhs, mixer_at(mixers, depth), preferred_element_type=F32)
            value = part if value is None else value + part
        rows = source.shape[1]
        return value[:rows], value[rows:]

    def gate_first(hidden, saved, side, index, slot):
        low = side.astype(F32)
        keep = jnp.concatenate([low, saved.astype(F32), low], axis=0) > 0
        ref.padded_two[index] = jnp.where(keep, hidden, 0.0)
        store_taps(ref.padded_two.at[index], taps_two, slot, 9 - LEAD, columns)

    lane = lax.broadcasted_iota(jnp.int32, (channels, merged), 1)
    sub = lax.broadcasted_iota(jnp.int32, (channels, merged), 0)
    diagonal = lax.rem(lane, channels) == sub
    table_lanes = cameras * row_count * row_count
    owner = lax.broadcasted_iota(
        jnp.int32, (cameras * row_count, table_lanes), 1
    ) // row_count == lax.broadcasted_iota(jnp.int32, (cameras * row_count, table_lanes), 0)

    def spread_rows(group):
        rows = [
            jnp.where(owner, ref.row_table[actual(group * GROUP + sphere)], 0.0)
            for sphere in range(GROUP)
        ]
        return jnp.dot(
            jnp.concatenate(rows, axis=0).astype(BF16),
            ref.expand[...],
            preferred_element_type=F32,
        )

    def mix_rows(spread, earlier):
        for camera in range(cameras):
            for sphere in range(GROUP):
                start = (sphere * cameras + camera) * row_count
                weights = jnp.concatenate(
                    [
                        jnp.where(diagonal, spread[start + r : start + r + 1], 0.0)
                        for r in range(row_count)
                    ],
                    axis=0,
                ).astype(BF16)
                value = jnp.dot(
                    volume[earlier + sphere], weights, preferred_element_type=F32
                ).astype(BF16)
                for block in range(blocks):
                    mixed[camera, block, sphere * VBLOCK : (sphere + 1) * VBLOCK] = value[
                        block * VBLOCK : (block + 1) * VBLOCK
                    ]

    width = GROUP * VBLOCK
    distance = (
        lax.rem(lax.broadcasted_iota(jnp.int32, (WINDOW, width), 1), VBLOCK)
        - lax.broadcasted_iota(jnp.int32, (WINDOW, width), 0)
        + (LEFT - LEAD)
    ).astype(F32)

    def tap_rows(group):
        quarter = lax.broadcasted_iota(jnp.int32, (spheres, width), 1) // VBLOCK
        chosen = lax.broadcasted_iota(jnp.int32, (spheres, width), 0) == actual(
            group * GROUP + quarter
        )
        return jnp.dot(
            ref.tap_table[...], chosen.astype(BF16), preferred_element_type=F32
        )

    def warp_columns(rows_all, first, last):
        for camera in range(first, last):
            rows = rows_all[camera * SLOT : (camera + 1) * SLOT]
            tap_of = distance - rows[TAPS : TAPS + 1]
            matrix = jnp.zeros((WINDOW, width), F32)
            for tap in range(TAPS):
                matrix = jnp.where(tap_of == float(tap), rows[tap : tap + 1], matrix)
            matrix = matrix.astype(BF16)
            for block in range(blocks):
                place = slice(block * VBLOCK, block * VBLOCK + WINDOW)
                total[camera, place] = total[camera, place] + jnp.dot(
                    matrix, mixed[camera, block], preferred_element_type=F32
                )

    @pl.when(step == 0)
    def _():
        from_table = lax.broadcasted_iota(jnp.int32, (table_lanes, merged), 0)
        to_lane = lax.broadcasted_iota(jnp.int32, (table_lanes, merged), 1)
        ref.expand[...] = jnp.where(
            lax.rem(from_table, row_count) == to_lane // channels, 1.0, 0.0
        ).astype(BF16)
        total[...] = jnp.zeros_like(total)
        volume[...] = jnp.zeros_like(volume)
        ref.spread[...] = jnp.zeros_like(ref.spread)
        ref.tap_rows[...] = jnp.zeros_like(ref.tap_rows)
        if paired:
            taps_one[2] = jnp.zeros_like(taps_one[2])
            taps_one[3] = jnp.zeros_like(taps_one[3])
        else:
            for index in range(2):
                gate_second(ref.low_rim[1 - index], ref.low_corner[1 - index], index, 2 + index)
        for index in range(2):
            place = inner(index)
            grad = masked(ref.cot_zero[place], ref.second_zero[place])
            gate_second(grad, side_of(index), 2 + index, index)
        order = (2, 3, 0, 1)
        for index in range(2):
            if index == 0 and paired:
                taps_two[0] = jnp.zeros_like(taps_two[0])
                continue
            hidden = jnp.zeros((wide, merged), F32)
            for depth in range(3):
                hidden = hidden + jnp.dot(
                    taps_one[order[index + 2 - depth]],
                    mixer_at(ref.mixer_second, depth),
                    preferred_element_type=F32,
                )
            if index == 0:
                gate_first(hidden, ref.low_rim[2], ref.low_corner[0], index, index)
            else:
                gate_first(hidden, ref.first_zero[0], side_of(0), index, index)

    first_sphere = step * (UNROLL * GROUP)
    for part in range(UNROLL):
        base = first_sphere + part * GROUP
        slot = part * GROUP
        final = last if part == UNROLL - 1 else None
        earlier = ((part - 1) % UNROLL) * GROUP
        for index in range(2):
            sphere = base + 2 + index
            gate_second(
                gated(sphere, first_sphere + 2), side_of(sphere), slot + index, slot + 2 + index
            )
        pair = conv(taps_one, ref.mixer_second, slot)
        for index in range(2):
            sphere = base + 1 + index
            saved = ref.first[inside(sphere, first_sphere + 1, ref.first.shape[0])]
            gate_first(pair[index], saved, side_of(sphere), slot + index, slot + 2 + index)
        for index in range(2):
            sphere = base + 4 + index
            grad, side = gated(sphere, first_sphere + 2), side_of(sphere)
            if final is not None:
                grad = jnp.where(final, ref.high_rim[index], grad)
                side = jnp.where(final, ref.high_corner[index], side)
            gate_second(grad, side, slot + 2 + index, slot + 4 + index)
        mix_rows(ref.spread, earlier)
        pair = conv(taps_one, ref.mixer_second, slot + 2)
        for index in range(2):
            sphere = base + 3 + index
            saved = ref.first[inside(sphere, first_sphere + 1, ref.first.shape[0])]
            side = side_of(sphere)
            if final is not None and index == 1:
                saved = jnp.where(final, ref.high_rim[2], saved)
                side = jnp.where(final, ref.high_corner[0], side)
            gate_first(pair[index], saved, side, slot + 2 + index, slot + 4 + index)
        for start in range(0, GROUP, 2):
            pair = conv(taps_two, ref.mixer_first, slot + start)
            for index in range(2):
                volume[slot + start + index] = pair[index].astype(BF16)
            warp_columns(ref.tap_rows, start * cameras // GROUP, (start + 2) * cameras // GROUP)
        ref.spread[...] = spread_rows(step * UNROLL + part)
        ref.tap_rows[...] = tap_rows(step * UNROLL + part)
    for slot in range(2):
        taps_one[slot] = taps_one[slot + UNROLL * GROUP]
        taps_two[slot] = taps_two[slot + UNROLL * GROUP]

    def joined(row):
        return jnp.concatenate(
            [
                total[camera, :, row * channels : (row + 1) * channels]
                for camera in range(cameras)
            ],
            axis=1,
        )

    @pl.when(last)
    def _():
        mix_rows(ref.spread, (UNROLL - 1) * GROUP)
        warp_columns(ref.tap_rows, 0, cameras)
        if not paired:
            for row in range(row_count):
                ref.whole[row] = joined(row)
            return
        half = row_count // 2
        own_high = ref.info[1] > 0
        for row in range(half):
            low, high = joined(row), joined(row + half)
            for mine, main, left, right in (
                (True, ref.own, ref.own_left, ref.own_right),
                (False, ref.peer, ref.peer_left, ref.peer_right),
            ):
                value = jnp.where(own_high, high, low) if mine else jnp.where(own_high, low, high)
                main[row] = value[LEFT : LEFT + columns].astype(main.dtype)
                left[row] = value[:LEFT].astype(BF16)
                right[row] = value[LEFT + columns :].astype(BF16)


def sweep(info, volumes, tables, row_count, cameras, paired):
    cot, second, first = volumes
    spheres, columns, merged = cot.shape
    groups = spheres // GROUP
    wide = columns + 16
    extended = columns + LEFT + RIGHT
    channels = merged // row_count
    half, lanes = row_count // 2, cameras * channels
    once = pl.Buffered(buffer_count=1)

    def whole(shape):
        zeros = (0,) * len(shape)
        return pl.BlockSpec(shape, lambda g, s: zeros, pipeline_mode=once)

    def spheres_from(ahead, count, **more):
        def index_map(g, s):
            return block_start(s[0], ahead(g), count, spheres), 0, 0

        shape = (pl.Element(count), pl.Element(columns), pl.Element(merged))
        return pl.BlockSpec(shape, index_map, **more)

    block = UNROLL * GROUP
    inputs = {name: (array, whole(array.shape)) for name, array in tables.items()}
    inputs.update(
        cot=(cot, spheres_from(lambda g: block * g + 2, block)),
        second=(second, spheres_from(lambda g: block * g + 2, block)),
        first=(first, spheres_from(lambda g: block * g + 1, block)),
        cot_zero=(cot, spheres_from(lambda g: 0, 2, pipeline_mode=once)),
        second_zero=(second, spheres_from(lambda g: 0, 2, pipeline_mode=once)),
        first_zero=(first, spheres_from(lambda g: 0, 1, pipeline_mode=once)),
    )
    if paired:
        outputs = dict(
            own=((half, columns, lanes), F32),
            own_left=((half, LEFT, lanes), BF16),
            own_right=((half, RIGHT, lanes), BF16),
            peer=((half, columns, lanes), BF16),
            peer_left=((half, LEFT, lanes), BF16),
            peer_right=((half, RIGHT, lanes), BF16),
        )
    else:
        outputs = dict(whole=((row_count, extended, lanes), F32))
    scratch = dict(
        taps_one=((block + 2, wide, 3 * merged), BF16),
        taps_two=((block + 2, columns, 3 * merged), BF16),
        padded_one=((block, columns + 32, merged), F32),
        padded_two=((block, wide, merged), F32),
        volume=((block, columns, merged), BF16),
        mixed=((cameras, columns // VBLOCK, GROUP * VBLOCK, merged), BF16),
        total=((cameras, extended, merged), F32),
        expand=((cameras * row_count * row_count, merged), BF16),
        spread=((GROUP * cameras * row_count, merged), F32),
        tap_rows=((cameras * SLOT, GROUP * VBLOCK), F32),
    )
    names = list(dict(info=0)) + list(inputs) + list(outputs) + list(scratch)
    flops = 2 * spheres * columns * merged * merged * (18 + cameras + cameras // 2)
    results = pl.pallas_call(
        functools.partial(sweep_kernel, names, row_count, paired),
        grid_spec=pltpu.PrefetchScalarGridSpec(
            num_scalar_prefetch=1,
            grid=(groups // UNROLL,),
            in_specs=[spec for _, spec in inputs.values()],
            out_specs=[whole(shape) for shape, _ in outputs.values()],
            scratch_shapes=[pltpu.VMEM(shape, kind) for shape, kind in scratch.values()],
        ),
        out_shape=[jax.ShapeDtypeStruct(shape, kind) for shape, kind in outputs.values()],
        compiler_params=pltpu.CompilerParams(
            dimension_semantics=(pltpu.ARBITRARY,), vmem_limit_bytes=56 * 2**20
        ),
        cost_estimate=pl.CostEstimate(
            flops=flops, bytes_accessed=3 * cot.size * 2, transcendentals=0
        ),
        name="sweep",
    )(info, *[array for array, _ in inputs.values()])
    return SimpleNamespace(**dict(zip(outputs, results)))


def finish_kernel(own, peer, own_start, own_end, peer_start, peer_end, out):
    columns = out.shape[1]
    out[...] = own[...] + peer[...].astype(F32)
    start, end = slice(0, RIGHT), slice(columns - LEFT, columns)
    out[:, start] = out[:, start] + (own_start[...].astype(F32) + peer_start[...].astype(F32))
    out[:, end] = out[:, end] + (own_end[...].astype(F32) + peer_end[...].astype(F32))


def row_mixers(kernel, row_count):
    channels = kernel.shape[3]
    strip = jnp.transpose(kernel, (0, 1, 4, 2, 3)).reshape(9, channels, 3 * channels)
    merged = row_count * channels
    strip = jnp.pad(strip, ((0, 0), (0, 0), (merged, merged)))
    rows = [
        lax.slice_in_dim(
            strip, merged - (row - 1) * channels, 2 * merged - (row - 1) * channels, axis=2
        )
        for row in range(row_count)
    ]
    return jnp.stack(rows, axis=1).reshape(3, 3 * merged, merged)


def ring(offset):
    count = lax.axis_size("azim")
    return [(i, (i + offset) % count) for i in range(count)]


def stride(offset):
    count = lax.axis_size("depth")
    if count == 2:
        return [(0, 1), (1, 0)]
    return [(i, i + offset) for i in range(count) if 0 <= i + offset < count]


def joint(depth_pairs, azim_pairs):
    width = lax.axis_size("azim")
    return [
        (d0 * width + a0, d1 * width + a1)
        for d0, d1 in depth_pairs
        for a0, a1 in azim_pairs
    ]


def body(cot, second, first, kernel_first, kernel_second, row_resample, col_taps, band_width, col_offset):
    spheres, columns, merged = cot.shape
    cameras, _, row_count, _ = row_resample.shape
    depth_index = lax.axis_index("depth").astype(jnp.int32)
    paired = lax.axis_size("depth") == 2
    both = ("depth", "azim")
    forward, backward = ring(1), ring(-1)
    tables = {}

    def send(offset, side):
        right, rim, corner = edges(jnp.full((1,), side, jnp.int32), cot, second, first)
        pairs = stride(offset)
        got_rim = lax.ppermute(rim, "depth", pairs)
        return right, got_rim, lax.ppermute(corner, both, joint(pairs, forward))

    if paired:
        right, high_rim, high_corner = send(-1, 1 - depth_index)
        flip = depth_index
    else:
        right, low_rim, low_corner = send(1, 1)
        _, high_rim, high_corner = send(-1, 0)
        tables.update(low_rim=low_rim, low_corner=low_corner)
        flip = jnp.zeros((), jnp.int32)
    info = jnp.stack([flip, depth_index])
    turned = lambda kernel: jnp.where(flip > 0, kernel[::-1], kernel)

    keep = lax.broadcasted_iota(jnp.int32, col_taps.shape, 2) < band_width[:, :, None]
    taps = jnp.where(keep, col_taps, 0.0)
    table = jnp.concatenate([taps, col_offset[:, :, None].astype(F32)], axis=2)
    table = jnp.pad(jnp.transpose(table, (0, 2, 1)), ((0, 0), (0, SLOT - TAPS - 1), (0, 0)))
    tables.update(
        high_rim=high_rim,
        high_corner=high_corner,
        from_left=lax.ppermute(right, "azim", forward),
        mixer_second=row_mixers(turned(kernel_second), row_count),
        mixer_first=row_mixers(turned(kernel_first), row_count),
        row_table=jnp.transpose(row_resample, (1, 0, 2, 3)).reshape(spheres, 1, -1),
        tap_table=table.reshape(cameras * SLOT, spheres).astype(BF16),
    )
    parts = sweep(info, (cot, second, first), tables, row_count, cameras, paired)

    if paired:
        swap = stride(1)
        got = (
            lax.ppermute(parts.peer, "depth", swap),
            lax.ppermute(parts.own_right, "azim", forward),
            lax.ppermute(parts.own_left, "azim", backward),
            lax.ppermute(parts.peer_right, both, joint(swap, forward)),
            lax.ppermute(parts.peer_left, both, joint(swap, backward)),
        )
        return pl.pallas_call(
            finish_kernel,
            out_shape=jax.ShapeDtypeStruct(parts.own.shape, F32),
            name="finish",
        )(parts.own, *got)
    partial = parts.whole
    at_end = lax.ppermute(partial[:, :LEFT], "azim", backward)
    at_start = lax.ppermute(partial[:, columns + LEFT :], "azim", forward)
    inner = partial[:, LEFT : columns + LEFT]
    inner = inner.at[:, columns - LEFT :].add(at_end)
    inner = inner.at[:, :RIGHT].add(at_start)
    return lax.psum_scatter(inner, "depth", scatter_dimension=0, tiled=True)


def solution(mesh):
    placed = (
        P("depth", "azim", None),
        P("depth", "azim", None),
        P("depth", "azim", None),
        P(),
        P(),
        P(None, "depth", None, None),
        P(None, "depth", None),
        P(None, "depth"),
        P(None, "depth"),
    )
    return jax.shard_map(
        body, mesh=mesh, in_specs=placed, out_specs=P("depth", "azim", None), check_vma=False
    )
```

```python
import functools
from types import SimpleNamespace

import jax
import jax.numpy as jnp
from jax import lax
from jax.experimental import pallas as pl
from jax.experimental.pallas import tpu as pltpu
from jax.sharding import PartitionSpec as P

TAPS = 8
SHIFT = 24
HALO = 4
LEAD = 2
LEFT = 40
RIGHT = 24
GROUP = 4
VBLOCK = 64
WINDOW = VBLOCK + LEFT + RIGHT
SLOT = 16
UNROLL = 1
BF16 = jnp.bfloat16
F32 = jnp.float32


def edge_kernel(
    side, cot_right, second_right, first_right, cot_rim, second_rim, first_rim, right, rim, corner
):
    spheres = cot_right.shape[0]
    gate = lambda cot, saved: jnp.where(saved > 0, cot, jnp.zeros_like(cot))
    top = side[0]
    for index in range(2):
        place = top + (1 - 2 * top) * index
        rim[index] = gate(cot_rim[place], second_rim[place])
    rim[2] = first_rim[0]
    last = slice(8 - HALO, 8)
    right[:, 0:HALO] = gate(cot_right[:, last], second_right[:, last])
    right[:, HALO : 2 * HALO] = first_right[:, last]
    for index in range(2):
        corner[index] = right[top * (spheres - 1) + (1 - 2 * top) * index]


def edges(side, cot, second, first):
    spheres, columns, merged = cot.shape
    pairs = spheres // 2
    high = pl.BlockSpec((spheres, 8, merged), lambda g, s: (0, columns // 8 - 1, 0))
    pair = pl.BlockSpec((2, columns, merged), lambda g, s: (s[0] * (pairs - 1), 0, 0))
    one = pl.BlockSpec((1, columns, merged), lambda g, s: (s[0] * (spheres - 1), 0, 0))
    shapes = ((spheres, 2 * HALO, merged), (3, columns, merged), (2, 2 * HALO, merged))
    return pl.pallas_call(
        edge_kernel,
        grid_spec=pltpu.PrefetchScalarGridSpec(
            num_scalar_prefetch=1,
            grid=(1,),
            in_specs=[high, high, high, pair, pair, one],
            out_specs=[pl.BlockSpec(s, lambda g, s: (0, 0, 0)) for s in shapes],
        ),
        out_shape=[jax.ShapeDtypeStruct(s, BF16) for s in shapes],
        name="edges",
    )(side, cot, second, first, cot, second, first)


def block_start(flip, sphere, count, spheres):
    sphere = jnp.minimum(sphere, spheres - count)
    return sphere + flip * (spheres - count - 2 * sphere)


def sweep_kernel(names, row_count, paired, *refs):
    ref = SimpleNamespace(**dict(zip(names, refs)))
    flip = ref.info[0]
    step = pl.program_id(0)
    last = step == pl.num_programs(0) - 1
    spheres, _, merged = ref.from_left.shape
    taps_one, taps_two = ref.taps_one, ref.taps_two
    columns = taps_two.shape[1]
    volume, mixed, total = ref.volume, ref.mixed, ref.total
    cameras = total.shape[0]
    channels = merged // row_count
    wide = columns + 16
    blocks = columns // VBLOCK
    actual = lambda v: flip * (spheres - 1) + (1 - 2 * flip) * v
    inner = lambda i: flip + (1 - 2 * flip) * i
    mixer_at = lambda mixers, depth: mixers[depth]

    def store_taps(source, target, slot, first_row, rows):
        for tap in range(3):
            target[slot % target.shape[0], :, tap * merged : (tap + 1) * merged] = source[
                first_row - tap : first_row - tap + rows
            ].astype(BF16)

    def gate_second(grad, side, index, slot):
        padded = ref.padded_one.at[index]
        padded[16 : 16 + columns] = grad.astype(F32)
        padded[16 - HALO : 16] = side[0:HALO].astype(F32)
        store_taps(padded, taps_one, slot, 9, wide)

    def masked(cot, saved):
        return jnp.where(saved > 0, cot, jnp.zeros_like(cot))

    def gated(v, first_sphere):
        place = inside(v, first_sphere, ref.cot.shape[0])
        return masked(ref.cot[place], ref.second[place])

    def inside(v, first_sphere, count):
        start = block_start(flip, first_sphere, count, spheres)
        return actual(jnp.minimum(v, spheres - 1)) - start

    def side_of(v):
        return ref.from_left[actual(jnp.minimum(v, spheres - 1))]

    def conv(source, mixers, slot):
        value = None
        for depth in (2, 1, 0):
            lhs = jnp.concatenate(
                [source[(slot + at - depth) % source.shape[0]] for at in (2, 3)], axis=0
            )
            part = jnp.dot(lhs, mixer_at(mixers, depth), preferred_element_type=F32)
            value = part if value is None else value + part
        rows = source.shape[1]
        return value[:rows], value[rows:]

    def gate_first(hidden, saved, side, index, slot):
        low = side.astype(F32)
        keep = jnp.concatenate([low, saved.astype(F32), low], axis=0) > 0
        ref.padded_two[index] = jnp.where(keep, hidden, 0.0)
        store_taps(ref.padded_two.at[index], taps_two, slot, 9 - LEAD, columns)

    lane = lax.broadcasted_iota(jnp.int32, (channels, merged), 1)
    sub = lax.broadcasted_iota(jnp.int32, (channels, merged), 0)
    diagonal = lax.rem(lane, channels) == sub
    table_lanes = cameras * row_count * row_count
    owner = lax.broadcasted_iota(
        jnp.int32, (cameras * row_count, table_lanes), 1
    ) // row_count == lax.broadcasted_iota(jnp.int32, (cameras * row_count, table_lanes), 0)

    def spread_rows(group):
        rows = [
            jnp.where(owner, ref.row_table[actual(group * GROUP + sphere)], 0.0)
            for sphere in range(GROUP)
        ]
        return jnp.dot(
            jnp.concatenate(rows, axis=0).astype(BF16),
            ref.expand[...],
            preferred_element_type=F32,
        )

    def mix_rows(spread, earlier):
        for camera in range(cameras):
            for sphere in range(GROUP):
                start = (sphere * cameras + camera) * row_count
                weights = jnp.concatenate(
                    [
                        jnp.where(diagonal, spread[start + r : start + r + 1], 0.0)
                        for r in range(row_count)
                    ],
                    axis=0,
                ).astype(BF16)
                value = jnp.dot(
                    volume[earlier + sphere], weights, preferred_element_type=F32
                ).astype(BF16)
                for block in range(blocks):
                    mixed[camera, block, sphere * VBLOCK : (sphere + 1) * VBLOCK] = value[
                        block * VBLOCK : (block + 1) * VBLOCK
                    ]

    width = GROUP * VBLOCK
    distance = (
        lax.rem(lax.broadcasted_iota(jnp.int32, (WINDOW, width), 1), VBLOCK)
        - lax.broadcasted_iota(jnp.int32, (WINDOW, width), 0)
        + (LEFT - LEAD)
    ).astype(F32)

    def tap_rows(group):
        quarter = lax.broadcasted_iota(jnp.int32, (spheres, width), 1) // VBLOCK
        chosen = lax.broadcasted_iota(jnp.int32, (spheres, width), 0) == actual(
            group * GROUP + quarter
        )
        return jnp.dot(
            ref.tap_table[...], chosen.astype(BF16), preferred_element_type=F32
        )

    def warp_columns(rows_all, first, last):
        for camera in range(first, last):
            rows = rows_all[camera * SLOT : (camera + 1) * SLOT]
            tap_of = distance - rows[TAPS : TAPS + 1]
            matrix = jnp.zeros((WINDOW, width), F32)
            for tap in range(TAPS):
                matrix = jnp.where(tap_of == float(tap), rows[tap : tap + 1], matrix)
            matrix = matrix.astype(BF16)
            for block in range(blocks):
                place = slice(block * VBLOCK, block * VBLOCK + WINDOW)
                total[camera, place] = total[camera, place] + jnp.dot(
                    matrix, mixed[camera, block], preferred_element_type=F32
                )

    @pl.when(step == 0)
    def _():
        from_table = lax.broadcasted_iota(jnp.int32, (table_lanes, merged), 0)
        to_lane = lax.broadcasted_iota(jnp.int32, (table_lanes, merged), 1)
        ref.expand[...] = jnp.where(
            lax.rem(from_table, row_count) == to_lane // channels, 1.0, 0.0
        ).astype(BF16)
        total[...] = jnp.zeros_like(total)
        volume[...] = jnp.zeros_like(volume)
        ref.spread[...] = jnp.zeros_like(ref.spread)
        ref.tap_rows[...] = jnp.zeros_like(ref.tap_rows)
        if paired:
            taps_one[2] = jnp.zeros_like(taps_one[2])
            taps_one[3] = jnp.zeros_like(taps_one[3])
        else:
            for index in range(2):
                gate_second(ref.low_rim[1 - index], ref.low_corner[1 - index], index, 2 + index)
        for index in range(2):
            place = inner(index)
            grad = masked(ref.cot_zero[place], ref.second_zero[place])
            gate_second(grad, side_of(index), 2 + index, index)
        order = (2, 3, 0, 1)
        for index in range(2):
            if index == 0 and paired:
                taps_two[0] = jnp.zeros_like(taps_two[0])
                continue
            hidden = jnp.zeros((wide, merged), F32)
            for depth in range(3):
                hidden = hidden + jnp.dot(
                    taps_one[order[index + 2 - depth]],
                    mixer_at(ref.mixer_second, depth),
                    preferred_element_type=F32,
                )
            if index == 0:
                gate_first(hidden, ref.low_rim[2], ref.low_corner[0], index, index)
            else:
                gate_first(hidden, ref.first_zero[0], side_of(0), index, index)

    first_sphere = step * (UNROLL * GROUP)
    for part in range(UNROLL):
        base = first_sphere + part * GROUP
        slot = part * GROUP
        final = last if part == UNROLL - 1 else None
        earlier = ((part - 1) % UNROLL) * GROUP
        for index in range(2):
            sphere = base + 2 + index
            gate_second(
                gated(sphere, first_sphere + 2), side_of(sphere), slot + index, slot + 2 + index
            )
        pair = conv(taps_one, ref.mixer_second, slot)
        for index in range(2):
            sphere = base + 1 + index
            saved = ref.first[inside(sphere, first_sphere + 1, ref.first.shape[0])]
            gate_first(pair[index], saved, side_of(sphere), slot + index, slot + 2 + index)
        for index in range(2):
            sphere = base + 4 + index
            grad, side = gated(sphere, first_sphere + 2), side_of(sphere)
            if final is not None:
                grad = jnp.where(final, ref.high_rim[index], grad)
                side = jnp.where(final, ref.high_corner[index], side)
            gate_second(grad, side, slot + 2 + index, slot + 4 + index)
        mix_rows(ref.spread, earlier)
        pair = conv(taps_one, ref.mixer_second, slot + 2)
        for index in range(2):
            sphere = base + 3 + index
            saved = ref.first[inside(sphere, first_sphere + 1, ref.first.shape[0])]
            side = side_of(sphere)
            if final is not None and index == 1:
                saved = jnp.where(final, ref.high_rim[2], saved)
                side = jnp.where(final, ref.high_corner[0], side)
            gate_first(pair[index], saved, side, slot + 2 + index, slot + 4 + index)
        for start in range(0, GROUP, 2):
            pair = conv(taps_two, ref.mixer_first, slot + start)
            for index in range(2):
                volume[slot + start + index] = pair[index].astype(BF16)
            warp_columns(ref.tap_rows, start * cameras // GROUP, (start + 2) * cameras // GROUP)
        ref.spread[...] = spread_rows(step * UNROLL + part)
        ref.tap_rows[...] = tap_rows(step * UNROLL + part)
    for slot in range(2):
        taps_two[slot] = taps_two[slot + UNROLL * GROUP]

    def joined(row):
        return jnp.concatenate(
            [
                total[camera, :, row * channels : (row + 1) * channels]
                for camera in range(cameras)
            ],
            axis=1,
        )

    @pl.when(last)
    def _():
        mix_rows(ref.spread, (UNROLL - 1) * GROUP)
        warp_columns(ref.tap_rows, 0, cameras)
        if not paired:
            for row in range(row_count):
                ref.whole[row] = joined(row)
            return
        half = row_count // 2
        own_high = ref.info[1] > 0
        for row in range(half):
            low, high = joined(row), joined(row + half)
            for mine, main, left, right in (
                (True, ref.own, ref.own_left, ref.own_right),
                (False, ref.peer, ref.peer_left, ref.peer_right),
            ):
                value = jnp.where(own_high, high, low) if mine else jnp.where(own_high, low, high)
                main[row] = value[LEFT : LEFT + columns].astype(main.dtype)
                left[row] = value[:LEFT].astype(BF16)
                right[row] = value[LEFT + columns :].astype(BF16)


def sweep(info, volumes, tables, row_count, cameras, paired):
    cot, second, first = volumes
    spheres, columns, merged = cot.shape
    groups = spheres // GROUP
    wide = columns + 16
    extended = columns + LEFT + RIGHT
    channels = merged // row_count
    half, lanes = row_count // 2, cameras * channels
    once = pl.Buffered(buffer_count=1)

    def whole(shape):
        zeros = (0,) * len(shape)
        return pl.BlockSpec(shape, lambda g, s: zeros, pipeline_mode=once)

    def spheres_from(ahead, count, **more):
        def index_map(g, s):
            return block_start(s[0], ahead(g), count, spheres), 0, 0

        shape = (pl.Element(count), pl.Element(columns), pl.Element(merged))
        return pl.BlockSpec(shape, index_map, **more)

    block = UNROLL * GROUP
    inputs = {name: (array, whole(array.shape)) for name, array in tables.items()}
    inputs.update(
        cot=(cot, spheres_from(lambda g: block * g + 2, block)),
        second=(second, spheres_from(lambda g: block * g + 2, block)),
        first=(first, spheres_from(lambda g: block * g + 1, block)),
        cot_zero=(cot, spheres_from(lambda g: 0, 2, pipeline_mode=once)),
        second_zero=(second, spheres_from(lambda g: 0, 2, pipeline_mode=once)),
        first_zero=(first, spheres_from(lambda g: 0, 1, pipeline_mode=once)),
    )
    if paired:
        outputs = dict(
            own=((half, columns, lanes), F32),
            own_left=((half, LEFT, lanes), BF16),
            own_right=((half, RIGHT, lanes), BF16),
            peer=((half, columns, lanes), BF16),
            peer_left=((half, LEFT, lanes), BF16),
            peer_right=((half, RIGHT, lanes), BF16),
        )
    else:
        outputs = dict(whole=((row_count, extended, lanes), F32))
    scratch = dict(
        taps_one=((GROUP, wide, 3 * merged), BF16),
        taps_two=((block + 2, columns, 3 * merged), BF16),
        padded_one=((block, columns + 32, merged), F32),
        padded_two=((block, wide, merged), F32),
        volume=((block, columns, merged), BF16),
        mixed=((cameras, columns // VBLOCK, GROUP * VBLOCK, merged), BF16),
        total=((cameras, extended, merged), F32),
        expand=((cameras * row_count * row_count, merged), BF16),
        spread=((GROUP * cameras * row_count, merged), F32),
        tap_rows=((cameras * SLOT, GROUP * VBLOCK), F32),
    )
    names = list(dict(info=0)) + list(inputs) + list(outputs) + list(scratch)
    flops = 2 * spheres * columns * merged * merged * (18 + cameras + cameras // 2)
    results = pl.pallas_call(
        functools.partial(sweep_kernel, names, row_count, paired),
        grid_spec=pltpu.PrefetchScalarGridSpec(
            num_scalar_prefetch=1,
            grid=(groups // UNROLL,),
            in_specs=[spec for _, spec in inputs.values()],
            out_specs=[whole(shape) for shape, _ in outputs.values()],
            scratch_shapes=[pltpu.VMEM(shape, kind) for shape, kind in scratch.values()],
        ),
        out_shape=[jax.ShapeDtypeStruct(shape, kind) for shape, kind in outputs.values()],
        compiler_params=pltpu.CompilerParams(
            dimension_semantics=(pltpu.ARBITRARY,), vmem_limit_bytes=30 * 2**20
        ),
        cost_estimate=pl.CostEstimate(
            flops=flops, bytes_accessed=3 * cot.size * 2, transcendentals=0
        ),
        name="sweep",
    )(info, *[array for array, _ in inputs.values()])
    return SimpleNamespace(**dict(zip(outputs, results)))


def finish_kernel(own, peer, own_start, own_end, peer_start, peer_end, out):
    columns = out.shape[1]
    out[...] = own[...] + peer[...].astype(F32)
    start, end = slice(0, RIGHT), slice(columns - LEFT, columns)
    out[:, start] = out[:, start] + (own_start[...].astype(F32) + peer_start[...].astype(F32))
    out[:, end] = out[:, end] + (own_end[...].astype(F32) + peer_end[...].astype(F32))


def row_mixers(kernel, row_count):
    channels = kernel.shape[3]
    strip = jnp.transpose(kernel, (0, 1, 4, 2, 3)).reshape(9, channels, 3 * channels)
    merged = row_count * channels
    strip = jnp.pad(strip, ((0, 0), (0, 0), (merged, merged)))
    rows = [
        lax.slice_in_dim(
            strip, merged - (row - 1) * channels, 2 * merged - (row - 1) * channels, axis=2
        )
        for row in range(row_count)
    ]
    return jnp.stack(rows, axis=1).reshape(3, 3 * merged, merged)


def ring(offset):
    count = lax.axis_size("azim")
    return [(i, (i + offset) % count) for i in range(count)]


def stride(offset):
    count = lax.axis_size("depth")
    if count == 2:
        return [(0, 1), (1, 0)]
    return [(i, i + offset) for i in range(count) if 0 <= i + offset < count]


def joint(depth_pairs, azim_pairs):
    width = lax.axis_size("azim")
    return [
        (d0 * width + a0, d1 * width + a1)
        for d0, d1 in depth_pairs
        for a0, a1 in azim_pairs
    ]


def body(cot, second, first, kernel_first, kernel_second, row_resample, col_taps, band_width, col_offset):
    spheres, columns, merged = cot.shape
    cameras, _, row_count, _ = row_resample.shape
    depth_index = lax.axis_index("depth").astype(jnp.int32)
    paired = lax.axis_size("depth") == 2
    both = ("depth", "azim")
    forward, backward = ring(1), ring(-1)
    tables = {}

    def send(offset, side):
        right, rim, corner = edges(jnp.full((1,), side, jnp.int32), cot, second, first)
        pairs = stride(offset)
        got_rim = lax.ppermute(rim, "depth", pairs)
        return right, got_rim, lax.ppermute(corner, both, joint(pairs, forward))

    if paired:
        right, high_rim, high_corner = send(-1, 1 - depth_index)
        flip = depth_index
    else:
        right, low_rim, low_corner = send(1, 1)
        _, high_rim, high_corner = send(-1, 0)
        tables.update(low_rim=low_rim, low_corner=low_corner)
        flip = jnp.zeros((), jnp.int32)
    info = jnp.stack([flip, depth_index])
    turned = lambda kernel: jnp.where(flip > 0, kernel[::-1], kernel)

    keep = lax.broadcasted_iota(jnp.int32, col_taps.shape, 2) < band_width[:, :, None]
    taps = jnp.where(keep, col_taps, 0.0)
    table = jnp.concatenate([taps, col_offset[:, :, None].astype(F32)], axis=2)
    table = jnp.pad(jnp.transpose(table, (0, 2, 1)), ((0, 0), (0, SLOT - TAPS - 1), (0, 0)))
    tables.update(
        high_rim=high_rim,
        high_corner=high_corner,
        from_left=lax.ppermute(right, "azim", forward),
        mixer_second=row_mixers(turned(kernel_second), row_count),
        mixer_first=row_mixers(turned(kernel_first), row_count),
        row_table=jnp.transpose(row_resample, (1, 0, 2, 3)).reshape(spheres, 1, -1),
        tap_table=table.reshape(cameras * SLOT, spheres).astype(BF16),
    )
    parts = sweep(info, (cot, second, first), tables, row_count, cameras, paired)

    if paired:
        swap = stride(1)
        got = (
            lax.ppermute(parts.peer, "depth", swap),
            lax.ppermute(parts.own_right, "azim", forward),
            lax.ppermute(parts.own_left, "azim", backward),
            lax.ppermute(parts.peer_right, both, joint(swap, forward)),
            lax.ppermute(parts.peer_left, both, joint(swap, backward)),
        )
        return pl.pallas_call(
            finish_kernel,
            out_shape=jax.ShapeDtypeStruct(parts.own.shape, F32),
            name="finish",
        )(parts.own, *got)
    partial = parts.whole
    at_end = lax.ppermute(partial[:, :LEFT], "azim", backward)
    at_start = lax.ppermute(partial[:, columns + LEFT :], "azim", forward)
    inner = partial[:, LEFT : columns + LEFT]
    inner = inner.at[:, columns - LEFT :].add(at_end)
    inner = inner.at[:, :RIGHT].add(at_start)
    return lax.psum_scatter(inner, "depth", scatter_dimension=0, tiled=True)


def solution(mesh):
    placed = (
        P("depth", "azim", None),
        P("depth", "azim", None),
        P("depth", "azim", None),
        P(),
        P(),
        P(None, "depth", None, None),
        P(None, "depth", None),
        P(None, "depth"),
        P(None, "depth"),
    )
    return jax.shard_map(
        body, mesh=mesh, in_specs=placed, out_specs=P("depth", "azim", None), check_vma=False
    )
```

```python
import functools
from types import SimpleNamespace

import jax
import jax.numpy as jnp
from jax import lax
from jax.experimental import pallas as pl
from jax.experimental.pallas import tpu as pltpu
from jax.sharding import PartitionSpec as P

TAPS = 8
SHIFT = 24
HALO = 4
LEAD = 2
LEFT = 40
RIGHT = 24
GROUP = 4
VBLOCK = 64
WINDOW = VBLOCK + LEFT + RIGHT
SLOT = 16
UNROLL = 1
BF16 = jnp.bfloat16
F32 = jnp.float32


def edge_kernel(
    side, cot_right, second_right, first_right, cot_rim, second_rim, first_rim, right, rim, corner
):
    spheres = cot_right.shape[0]
    gate = lambda cot, saved: jnp.where(saved > 0, cot, jnp.zeros_like(cot))
    top = side[0]
    for index in range(2):
        place = top + (1 - 2 * top) * index
        rim[index] = gate(cot_rim[place], second_rim[place])
    rim[2] = first_rim[0]
    last = slice(8 - HALO, 8)
    right[:, 0:HALO] = gate(cot_right[:, last], second_right[:, last])
    right[:, HALO : 2 * HALO] = first_right[:, last]
    for index in range(2):
        corner[index] = right[top * (spheres - 1) + (1 - 2 * top) * index]


def edges(side, cot, second, first):
    spheres, columns, merged = cot.shape
    pairs = spheres // 2
    high = pl.BlockSpec((spheres, 8, merged), lambda g, s: (0, columns // 8 - 1, 0))
    pair = pl.BlockSpec((2, columns, merged), lambda g, s: (s[0] * (pairs - 1), 0, 0))
    one = pl.BlockSpec((1, columns, merged), lambda g, s: (s[0] * (spheres - 1), 0, 0))
    shapes = ((spheres, 2 * HALO, merged), (3, columns, merged), (2, 2 * HALO, merged))
    return pl.pallas_call(
        edge_kernel,
        grid_spec=pltpu.PrefetchScalarGridSpec(
            num_scalar_prefetch=1,
            grid=(1,),
            in_specs=[high, high, high, pair, pair, one],
            out_specs=[pl.BlockSpec(s, lambda g, s: (0, 0, 0)) for s in shapes],
        ),
        out_shape=[jax.ShapeDtypeStruct(s, BF16) for s in shapes],
        name="edges",
    )(side, cot, second, first, cot, second, first)


def block_start(flip, sphere, count, spheres):
    sphere = jnp.minimum(sphere, spheres - count)
    return sphere + flip * (spheres - count - 2 * sphere)


def sweep_kernel(names, row_count, paired, *refs):
    ref = SimpleNamespace(**dict(zip(names, refs)))
    flip = ref.info[0]
    step = pl.program_id(0)
    last = step == pl.num_programs(0) - 1
    spheres, _, merged = ref.from_left.shape
    taps_one, taps_two = ref.taps_one, ref.taps_two
    columns = taps_two.shape[1]
    volume, mixed, total = ref.volume, ref.mixed, ref.total
    cameras = total.shape[0]
    channels = merged // row_count
    wide = columns + 16
    blocks = columns // VBLOCK
    actual = lambda v: flip * (spheres - 1) + (1 - 2 * flip) * v
    inner = lambda i: flip + (1 - 2 * flip) * i
    mixer_at = lambda mixers, depth: mixers[depth]

    def store_taps(source, target, slot, first_row, rows):
        for tap in range(3):
            target[slot % target.shape[0], :, tap * merged : (tap + 1) * merged] = source[
                first_row - tap : first_row - tap + rows
            ].astype(BF16)

    def gate_second(grad, side, index, slot):
        padded = ref.padded_one.at[index]
        padded[16 : 16 + columns] = grad.astype(F32)
        padded[16 - HALO : 16] = side[0:HALO].astype(F32)
        store_taps(padded, taps_one, slot, 9, wide)

    def gated(v, first_sphere):
        return ref.second[inside(v, first_sphere, ref.second.shape[0])]

    def inside(v, first_sphere, count):
        start = block_start(flip, first_sphere, count, spheres)
        return actual(jnp.minimum(v, spheres - 1)) - start

    def side_of(v):
        return ref.from_left[actual(jnp.minimum(v, spheres - 1))]

    def conv(source, mixers, slot):
        value = None
        for depth in (2, 1, 0):
            lhs = jnp.concatenate(
                [source[(slot + at - depth) % source.shape[0]] for at in (2, 3)], axis=0
            )
            part = jnp.dot(lhs, mixer_at(mixers, depth), preferred_element_type=F32)
            value = part if value is None else value + part
        rows = source.shape[1]
        return value[:rows], value[rows:]

    def gate_first(hidden, saved, side, index, slot):
        low = side.astype(F32)
        keep = jnp.concatenate([low, saved.astype(F32), low], axis=0) > 0
        ref.padded_two[index] = jnp.where(keep, hidden, 0.0)
        store_taps(ref.padded_two.at[index], taps_two, slot, 9 - LEAD, columns)

    lane = lax.broadcasted_iota(jnp.int32, (channels, merged), 1)
    sub = lax.broadcasted_iota(jnp.int32, (channels, merged), 0)
    diagonal = lax.rem(lane, channels) == sub
    table_lanes = cameras * row_count * row_count
    owner = lax.broadcasted_iota(
        jnp.int32, (cameras * row_count, table_lanes), 1
    ) // row_count == lax.broadcasted_iota(jnp.int32, (cameras * row_count, table_lanes), 0)

    def spread_rows(group):
        rows = [
            jnp.where(owner, ref.row_table[actual(group * GROUP + sphere)], 0.0)
            for sphere in range(GROUP)
        ]
        return jnp.dot(
            jnp.concatenate(rows, axis=0).astype(BF16),
            ref.expand[...],
            preferred_element_type=F32,
        )

    def mix_rows(spread, earlier):
        for camera in range(cameras):
            for sphere in range(GROUP):
                start = (sphere * cameras + camera) * row_count
                weights = jnp.concatenate(
                    [
                        jnp.where(diagonal, spread[start + r : start + r + 1], 0.0)
                        for r in range(row_count)
                    ],
                    axis=0,
                ).astype(BF16)
                value = jnp.dot(
                    volume[earlier + sphere], weights, preferred_element_type=F32
                ).astype(BF16)
                for block in range(blocks):
                    mixed[camera, block, sphere * VBLOCK : (sphere + 1) * VBLOCK] = value[
                        block * VBLOCK : (block + 1) * VBLOCK
                    ]

    width = GROUP * VBLOCK
    distance = (
        lax.rem(lax.broadcasted_iota(jnp.int32, (WINDOW, width), 1), VBLOCK)
        - lax.broadcasted_iota(jnp.int32, (WINDOW, width), 0)
        + (LEFT - LEAD)
    ).astype(F32)

    def tap_rows(group):
        quarter = lax.broadcasted_iota(jnp.int32, (spheres, width), 1) // VBLOCK
        chosen = lax.broadcasted_iota(jnp.int32, (spheres, width), 0) == actual(
            group * GROUP + quarter
        )
        return jnp.dot(
            ref.tap_table[...], chosen.astype(BF16), preferred_element_type=F32
        )

    def warp_columns(rows_all, first, last):
        for camera in range(first, last):
            rows = rows_all[camera * SLOT : (camera + 1) * SLOT]
            tap_of = distance - rows[TAPS : TAPS + 1]
            matrix = jnp.zeros((WINDOW, width), F32)
            for tap in range(TAPS):
                matrix = jnp.where(tap_of == float(tap), rows[tap : tap + 1], matrix)
            matrix = matrix.astype(BF16)
            for block in range(blocks):
                place = slice(block * VBLOCK, block * VBLOCK + WINDOW)
                total[camera, place] = total[camera, place] + jnp.dot(
                    matrix, mixed[camera, block], preferred_element_type=F32
                )

    @pl.when(step == 0)
    def _():
        from_table = lax.broadcasted_iota(jnp.int32, (table_lanes, merged), 0)
        to_lane = lax.broadcasted_iota(jnp.int32, (table_lanes, merged), 1)
        ref.expand[...] = jnp.where(
            lax.rem(from_table, row_count) == to_lane // channels, 1.0, 0.0
        ).astype(BF16)
        total[...] = jnp.zeros_like(total)
        volume[...] = jnp.zeros_like(volume)
        ref.spread[...] = jnp.zeros_like(ref.spread)
        ref.tap_rows[...] = jnp.zeros_like(ref.tap_rows)
        if paired:
            taps_one[2] = jnp.zeros_like(taps_one[2])
            taps_one[3] = jnp.zeros_like(taps_one[3])
        else:
            for index in range(2):
                gate_second(ref.low_rim[1 - index], ref.low_corner[1 - index], index, 2 + index)
        for index in range(2):
            place = inner(index)
            gate_second(ref.second_zero[place], side_of(index), 2 + index, index)
        order = (2, 3, 0, 1)
        for index in range(2):
            if index == 0 and paired:
                taps_two[0] = jnp.zeros_like(taps_two[0])
                continue
            hidden = jnp.zeros((wide, merged), F32)
            for depth in range(3):
                hidden = hidden + jnp.dot(
                    taps_one[order[index + 2 - depth]],
                    mixer_at(ref.mixer_second, depth),
                    preferred_element_type=F32,
                )
            if index == 0:
                gate_first(hidden, ref.low_rim[2], ref.low_corner[0], index, index)
            else:
                gate_first(hidden, ref.first_zero[0], side_of(0), index, index)

    first_sphere = step * (UNROLL * GROUP)
    for part in range(UNROLL):
        base = first_sphere + part * GROUP
        slot = part * GROUP
        final = last if part == UNROLL - 1 else None
        earlier = ((part - 1) % UNROLL) * GROUP
        for index in range(2):
            sphere = base + 2 + index
            gate_second(
                gated(sphere, first_sphere + 2), side_of(sphere), slot + index, slot + 2 + index
            )
        pair = conv(taps_one, ref.mixer_second, slot)
        for index in range(2):
            sphere = base + 1 + index
            saved = ref.first[inside(sphere, first_sphere + 1, ref.first.shape[0])]
            gate_first(pair[index], saved, side_of(sphere), slot + index, slot + 2 + index)
        for index in range(2):
            sphere = base + 4 + index
            grad, side = gated(sphere, first_sphere + 2), side_of(sphere)
            if final is not None:
                grad = jnp.where(final, ref.high_rim[index], grad)
                side = jnp.where(final, ref.high_corner[index], side)
            gate_second(grad, side, slot + 2 + index, slot + 4 + index)
        mix_rows(ref.spread, earlier)
        pair = conv(taps_one, ref.mixer_second, slot + 2)
        for index in range(2):
            sphere = base + 3 + index
            saved = ref.first[inside(sphere, first_sphere + 1, ref.first.shape[0])]
            side = side_of(sphere)
            if final is not None and index == 1:
                saved = jnp.where(final, ref.high_rim[2], saved)
                side = jnp.where(final, ref.high_corner[0], side)
            gate_first(pair[index], saved, side, slot + 2 + index, slot + 4 + index)
        for start in range(0, GROUP, 2):
            pair = conv(taps_two, ref.mixer_first, slot + start)
            for index in range(2):
                volume[slot + start + index] = pair[index].astype(BF16)
            warp_columns(ref.tap_rows, start * cameras // GROUP, (start + 2) * cameras // GROUP)
        ref.spread[...] = spread_rows(step * UNROLL + part)
        ref.tap_rows[...] = tap_rows(step * UNROLL + part)
    for slot in range(2):
        taps_two[slot] = taps_two[slot + UNROLL * GROUP]

    def joined(row):
        return jnp.concatenate(
            [
                total[camera, :, row * channels : (row + 1) * channels]
                for camera in range(cameras)
            ],
            axis=1,
        )

    @pl.when(last)
    def _():
        mix_rows(ref.spread, (UNROLL - 1) * GROUP)
        warp_columns(ref.tap_rows, 0, cameras)
        if not paired:
            for row in range(row_count):
                ref.whole[row] = joined(row)
            return
        half = row_count // 2
        own_high = ref.info[1] > 0
        for row in range(half):
            low, high = joined(row), joined(row + half)
            for mine, main, left, right in (
                (True, ref.own, ref.own_left, ref.own_right),
                (False, ref.peer, ref.peer_left, ref.peer_right),
            ):
                value = jnp.where(own_high, high, low) if mine else jnp.where(own_high, low, high)
                main[row] = value[LEFT : LEFT + columns].astype(main.dtype)
                left[row] = value[:LEFT].astype(BF16)
                right[row] = value[LEFT + columns :].astype(BF16)


def sweep(info, volumes, tables, row_count, cameras, paired):
    second, first = volumes
    spheres, columns, merged = second.shape
    groups = spheres // GROUP
    wide = columns + 16
    extended = columns + LEFT + RIGHT
    channels = merged // row_count
    half, lanes = row_count // 2, cameras * channels
    once = pl.Buffered(buffer_count=1)

    def whole(shape):
        zeros = (0,) * len(shape)
        return pl.BlockSpec(shape, lambda g, s: zeros, pipeline_mode=once)

    def spheres_from(ahead, count, **more):
        def index_map(g, s):
            return block_start(s[0], ahead(g), count, spheres), 0, 0

        shape = (pl.Element(count), pl.Element(columns), pl.Element(merged))
        return pl.BlockSpec(shape, index_map, **more)

    block = UNROLL * GROUP
    inputs = {name: (array, whole(array.shape)) for name, array in tables.items()}
    inputs.update(
        second=(second, spheres_from(lambda g: block * g + 2, block)),
        first=(first, spheres_from(lambda g: block * g + 1, block)),
        second_zero=(second, spheres_from(lambda g: 0, 2, pipeline_mode=once)),
        first_zero=(first, spheres_from(lambda g: 0, 1, pipeline_mode=once)),
    )
    if paired:
        outputs = dict(
            own=((half, columns, lanes), F32),
            own_left=((half, LEFT, lanes), BF16),
            own_right=((half, RIGHT, lanes), BF16),
            peer=((half, columns, lanes), BF16),
            peer_left=((half, LEFT, lanes), BF16),
            peer_right=((half, RIGHT, lanes), BF16),
        )
    else:
        outputs = dict(whole=((row_count, extended, lanes), F32))
    scratch = dict(
        taps_one=((GROUP, wide, 3 * merged), BF16),
        taps_two=((block + 2, columns, 3 * merged), BF16),
        padded_one=((block, columns + 32, merged), F32),
        padded_two=((block, wide, merged), F32),
        volume=((block, columns, merged), BF16),
        mixed=((cameras, columns // VBLOCK, GROUP * VBLOCK, merged), BF16),
        total=((cameras, extended, merged), F32),
        expand=((cameras * row_count * row_count, merged), BF16),
        spread=((GROUP * cameras * row_count, merged), F32),
        tap_rows=((cameras * SLOT, GROUP * VBLOCK), F32),
    )
    names = list(dict(info=0)) + list(inputs) + list(outputs) + list(scratch)
    flops = 2 * spheres * columns * merged * merged * (18 + cameras + cameras // 2)
    results = pl.pallas_call(
        functools.partial(sweep_kernel, names, row_count, paired),
        grid_spec=pltpu.PrefetchScalarGridSpec(
            num_scalar_prefetch=1,
            grid=(groups // UNROLL,),
            in_specs=[spec for _, spec in inputs.values()],
            out_specs=[whole(shape) for shape, _ in outputs.values()],
            scratch_shapes=[pltpu.VMEM(shape, kind) for shape, kind in scratch.values()],
        ),
        out_shape=[jax.ShapeDtypeStruct(shape, kind) for shape, kind in outputs.values()],
        compiler_params=pltpu.CompilerParams(
            dimension_semantics=(pltpu.ARBITRARY,), vmem_limit_bytes=46 * 2**20
        ),
        cost_estimate=pl.CostEstimate(
            flops=flops, bytes_accessed=2 * second.size * 2, transcendentals=0
        ),
        name="sweep",
    )(info, *[array for array, _ in inputs.values()])
    return SimpleNamespace(**dict(zip(outputs, results)))


def finish_kernel(own, peer, own_start, own_end, peer_start, peer_end, out):
    columns = out.shape[1]
    out[...] = own[...] + peer[...].astype(F32)
    start, end = slice(0, RIGHT), slice(columns - LEFT, columns)
    out[:, start] = out[:, start] + (own_start[...].astype(F32) + peer_start[...].astype(F32))
    out[:, end] = out[:, end] + (own_end[...].astype(F32) + peer_end[...].astype(F32))


def row_mixers(kernel, row_count):
    channels = kernel.shape[3]
    strip = jnp.transpose(kernel, (0, 1, 4, 2, 3)).reshape(9, channels, 3 * channels)
    merged = row_count * channels
    strip = jnp.pad(strip, ((0, 0), (0, 0), (merged, merged)))
    rows = [
        lax.slice_in_dim(
            strip, merged - (row - 1) * channels, 2 * merged - (row - 1) * channels, axis=2
        )
        for row in range(row_count)
    ]
    return jnp.stack(rows, axis=1).reshape(3, 3 * merged, merged)


def ring(offset):
    count = lax.axis_size("azim")
    return [(i, (i + offset) % count) for i in range(count)]


def stride(offset):
    count = lax.axis_size("depth")
    if count == 2:
        return [(0, 1), (1, 0)]
    return [(i, i + offset) for i in range(count) if 0 <= i + offset < count]


def joint(depth_pairs, azim_pairs):
    width = lax.axis_size("azim")
    return [
        (d0 * width + a0, d1 * width + a1)
        for d0, d1 in depth_pairs
        for a0, a1 in azim_pairs
    ]


def body(cot, second, first, kernel_first, kernel_second, row_resample, col_taps, band_width, col_offset):
    spheres, columns, merged = cot.shape
    cameras, _, row_count, _ = row_resample.shape
    depth_index = lax.axis_index("depth").astype(jnp.int32)
    paired = lax.axis_size("depth") == 2
    both = ("depth", "azim")
    forward, backward = ring(1), ring(-1)
    tables = {}

    def send(offset, side):
        right, rim, corner = edges(jnp.full((1,), side, jnp.int32), cot, second, first)
        pairs = stride(offset)
        got_rim = lax.ppermute(rim, "depth", pairs)
        return right, got_rim, lax.ppermute(corner, both, joint(pairs, forward))

    if paired:
        right, high_rim, high_corner = send(-1, 1 - depth_index)
        flip = depth_index
    else:
        right, low_rim, low_corner = send(1, 1)
        _, high_rim, high_corner = send(-1, 0)
        tables.update(low_rim=low_rim, low_corner=low_corner)
        flip = jnp.zeros((), jnp.int32)
    info = jnp.stack([flip, depth_index])
    turned = lambda kernel: jnp.where(flip > 0, kernel[::-1], kernel)

    keep = lax.broadcasted_iota(jnp.int32, col_taps.shape, 2) < band_width[:, :, None]
    taps = jnp.where(keep, col_taps, 0.0)
    table = jnp.concatenate([taps, col_offset[:, :, None].astype(F32)], axis=2)
    table = jnp.pad(jnp.transpose(table, (0, 2, 1)), ((0, 0), (0, SLOT - TAPS - 1), (0, 0)))
    tables.update(
        high_rim=high_rim,
        high_corner=high_corner,
        from_left=lax.ppermute(right, "azim", forward),
        mixer_second=row_mixers(turned(kernel_second), row_count),
        mixer_first=row_mixers(turned(kernel_first), row_count),
        row_table=jnp.transpose(row_resample, (1, 0, 2, 3)).reshape(spheres, 1, -1),
        tap_table=table.reshape(cameras * SLOT, spheres).astype(BF16),
    )
    second_grad = jnp.where(second > 0, cot, jnp.zeros_like(cot))
    parts = sweep(info, (second_grad, first), tables, row_count, cameras, paired)

    if paired:
        swap = stride(1)
        got = (
            lax.ppermute(parts.peer, "depth", swap),
            lax.ppermute(parts.own_right, "azim", forward),
            lax.ppermute(parts.own_left, "azim", backward),
            lax.ppermute(parts.peer_right, both, joint(swap, forward)),
            lax.ppermute(parts.peer_left, both, joint(swap, backward)),
        )
        return pl.pallas_call(
            finish_kernel,
            out_shape=jax.ShapeDtypeStruct(parts.own.shape, F32),
            name="finish",
        )(parts.own, *got)
    partial = parts.whole
    at_end = lax.ppermute(partial[:, :LEFT], "azim", backward)
    at_start = lax.ppermute(partial[:, columns + LEFT :], "azim", forward)
    inner = partial[:, LEFT : columns + LEFT]
    inner = inner.at[:, columns - LEFT :].add(at_end)
    inner = inner.at[:, :RIGHT].add(at_start)
    return lax.psum_scatter(inner, "depth", scatter_dimension=0, tiled=True)


def solution(mesh):
    placed = (
        P("depth", "azim", None),
        P("depth", "azim", None),
        P("depth", "azim", None),
        P(),
        P(),
        P(None, "depth", None, None),
        P(None, "depth", None),
        P(None, "depth"),
        P(None, "depth"),
    )
    return jax.shard_map(
        body, mesh=mesh, in_specs=placed, out_specs=P("depth", "azim", None), check_vma=False
    )
```

```python
import functools
from types import SimpleNamespace

import jax
import jax.numpy as jnp
from jax import lax
from jax.experimental import pallas as pl
from jax.experimental.pallas import tpu as pltpu
from jax.sharding import PartitionSpec as P

TAPS = 8
SHIFT = 24
HALO = 4
LEAD = 2
LEFT = 40
RIGHT = 24
GROUP = 4
VBLOCK = 64
WINDOW = VBLOCK + LEFT + RIGHT
SLOT = 16
UNROLL = 1
BF16 = jnp.bfloat16
F32 = jnp.float32


def edge_kernel(
    side, cot_right, second_right, first_right, cot_rim, second_rim, first_rim, right, rim, corner
):
    spheres = cot_right.shape[0]
    gate = lambda cot, saved: jnp.where(saved > 0, cot, jnp.zeros_like(cot))
    top = side[0]
    for index in range(2):
        place = top + (1 - 2 * top) * index
        rim[index] = gate(cot_rim[place], second_rim[place])
    rim[2] = first_rim[0]
    last = slice(8 - HALO, 8)
    right[:, 0:HALO] = gate(cot_right[:, last], second_right[:, last])
    right[:, HALO : 2 * HALO] = first_right[:, last]
    for index in range(2):
        corner[index] = right[top * (spheres - 1) + (1 - 2 * top) * index]


def edges(side, cot, second, first):
    spheres, columns, merged = cot.shape
    pairs = spheres // 2
    high = pl.BlockSpec((spheres, 8, merged), lambda g, s: (0, columns // 8 - 1, 0))
    pair = pl.BlockSpec((2, columns, merged), lambda g, s: (s[0] * (pairs - 1), 0, 0))
    one = pl.BlockSpec((1, columns, merged), lambda g, s: (s[0] * (spheres - 1), 0, 0))
    shapes = ((spheres, 2 * HALO, merged), (3, columns, merged), (2, 2 * HALO, merged))
    return pl.pallas_call(
        edge_kernel,
        grid_spec=pltpu.PrefetchScalarGridSpec(
            num_scalar_prefetch=1,
            grid=(1,),
            in_specs=[high, high, high, pair, pair, one],
            out_specs=[pl.BlockSpec(s, lambda g, s: (0, 0, 0)) for s in shapes],
        ),
        out_shape=[jax.ShapeDtypeStruct(s, BF16) for s in shapes],
        name="edges",
    )(side, cot, second, first, cot, second, first)


def gate_kernel(cot, second, out):
    size = cot.shape[0]
    place = pl.ds(pl.program_id(0) * size, size)
    out[place] = jnp.where(second[...] > 0, cot[...], jnp.zeros_like(cot))


def gate_all(cot, second):
    spheres, columns, merged = cot.shape
    block = pl.BlockSpec((GROUP, columns, merged), lambda g: (g, 0, 0))
    return pl.pallas_call(
        gate_kernel,
        grid=(spheres // GROUP,),
        in_specs=[block, block],
        out_specs=pl.BlockSpec(memory_space=pltpu.VMEM),
        out_shape=pltpu.VMEM(cot.shape, BF16),
        compiler_params=pltpu.CompilerParams(vmem_limit_bytes=48 * 2**20),
        cost_estimate=pl.CostEstimate(
            flops=cot.size, bytes_accessed=6 * cot.size, transcendentals=0
        ),
        name="gate",
    )(cot, second)


def block_start(flip, sphere, count, spheres):
    sphere = jnp.minimum(sphere, spheres - count)
    return sphere + flip * (spheres - count - 2 * sphere)


def sweep_kernel(names, row_count, paired, *refs):
    ref = SimpleNamespace(**dict(zip(names, refs)))
    flip = ref.info[0]
    step = pl.program_id(0)
    last = step == pl.num_programs(0) - 1
    spheres, _, merged = ref.from_left.shape
    taps_one, taps_two = ref.taps_one, ref.taps_two
    columns = taps_two.shape[1]
    volume, mixed, total = ref.volume, ref.mixed, ref.total
    cameras = total.shape[0]
    channels = merged // row_count
    wide = columns + 16
    blocks = columns // VBLOCK
    actual = lambda v: flip * (spheres - 1) + (1 - 2 * flip) * v
    inner = lambda i: flip + (1 - 2 * flip) * i
    mixer_at = lambda mixers, depth: mixers[depth]

    def store_taps(source, target, slot, first_row, rows):
        for tap in range(3):
            target[slot % target.shape[0], :, tap * merged : (tap + 1) * merged] = source[
                first_row - tap : first_row - tap + rows
            ].astype(BF16)

    def gate_second(grad, side, index, slot):
        padded = ref.padded_one.at[index]
        padded[16 : 16 + columns] = grad.astype(F32)
        padded[16 - HALO : 16] = side[0:HALO].astype(F32)
        store_taps(padded, taps_one, slot, 9, wide)

    def gated(v, first_sphere):
        return ref.second[inside(v, first_sphere, ref.second.shape[0])]

    def inside(v, first_sphere, count):
        start = block_start(flip, first_sphere, count, spheres)
        return actual(jnp.minimum(v, spheres - 1)) - start

    def side_of(v):
        return ref.from_left[actual(jnp.minimum(v, spheres - 1))]

    def conv(source, mixers, slot):
        value = None
        for depth in (2, 1, 0):
            lhs = jnp.concatenate(
                [source[(slot + at - depth) % source.shape[0]] for at in (2, 3)], axis=0
            )
            part = jnp.dot(lhs, mixer_at(mixers, depth), preferred_element_type=F32)
            value = part if value is None else value + part
        rows = source.shape[1]
        return value[:rows], value[rows:]

    def gate_first(hidden, saved, side, index, slot):
        low = side.astype(F32)
        keep = jnp.concatenate([low, saved.astype(F32), low], axis=0) > 0
        ref.padded_two[index] = jnp.where(keep, hidden, 0.0)
        store_taps(ref.padded_two.at[index], taps_two, slot, 9 - LEAD, columns)

    lane = lax.broadcasted_iota(jnp.int32, (channels, merged), 1)
    sub = lax.broadcasted_iota(jnp.int32, (channels, merged), 0)
    diagonal = lax.rem(lane, channels) == sub
    table_lanes = cameras * row_count * row_count
    owner = lax.broadcasted_iota(
        jnp.int32, (cameras * row_count, table_lanes), 1
    ) // row_count == lax.broadcasted_iota(jnp.int32, (cameras * row_count, table_lanes), 0)

    def spread_rows(group):
        rows = [
            jnp.where(owner, ref.row_table[actual(group * GROUP + sphere)], 0.0)
            for sphere in range(GROUP)
        ]
        return jnp.dot(
            jnp.concatenate(rows, axis=0).astype(BF16),
            ref.expand[...],
            preferred_element_type=F32,
        )

    def mix_rows(spread, earlier):
        for camera in range(cameras):
            for sphere in range(GROUP):
                start = (sphere * cameras + camera) * row_count
                weights = jnp.concatenate(
                    [
                        jnp.where(diagonal, spread[start + r : start + r + 1], 0.0)
                        for r in range(row_count)
                    ],
                    axis=0,
                ).astype(BF16)
                value = jnp.dot(
                    volume[earlier + sphere], weights, preferred_element_type=F32
                ).astype(BF16)
                for block in range(blocks):
                    mixed[camera, block, sphere * VBLOCK : (sphere + 1) * VBLOCK] = value[
                        block * VBLOCK : (block + 1) * VBLOCK
                    ]

    width = GROUP * VBLOCK
    distance = (
        lax.rem(lax.broadcasted_iota(jnp.int32, (WINDOW, width), 1), VBLOCK)
        - lax.broadcasted_iota(jnp.int32, (WINDOW, width), 0)
        + (LEFT - LEAD)
    ).astype(F32)

    def tap_rows(group):
        quarter = lax.broadcasted_iota(jnp.int32, (spheres, width), 1) // VBLOCK
        chosen = lax.broadcasted_iota(jnp.int32, (spheres, width), 0) == actual(
            group * GROUP + quarter
        )
        return jnp.dot(
            ref.tap_table[...], chosen.astype(BF16), preferred_element_type=F32
        )

    def warp_columns(rows_all, first, last):
        for camera in range(first, last):
            rows = rows_all[camera * SLOT : (camera + 1) * SLOT]
            tap_of = distance - rows[TAPS : TAPS + 1]
            matrix = jnp.zeros((WINDOW, width), F32)
            for tap in range(TAPS):
                matrix = jnp.where(tap_of == float(tap), rows[tap : tap + 1], matrix)
            matrix = matrix.astype(BF16)
            for block in range(blocks):
                place = slice(block * VBLOCK, block * VBLOCK + WINDOW)
                total[camera, place] = total[camera, place] + jnp.dot(
                    matrix, mixed[camera, block], preferred_element_type=F32
                )

    @pl.when(step == 0)
    def _():
        from_table = lax.broadcasted_iota(jnp.int32, (table_lanes, merged), 0)
        to_lane = lax.broadcasted_iota(jnp.int32, (table_lanes, merged), 1)
        ref.expand[...] = jnp.where(
            lax.rem(from_table, row_count) == to_lane // channels, 1.0, 0.0
        ).astype(BF16)
        total[...] = jnp.zeros_like(total)
        volume[...] = jnp.zeros_like(volume)
        ref.spread[...] = jnp.zeros_like(ref.spread)
        ref.tap_rows[...] = jnp.zeros_like(ref.tap_rows)
        if paired:
            taps_one[2] = jnp.zeros_like(taps_one[2])
            taps_one[3] = jnp.zeros_like(taps_one[3])
        else:
            for index in range(2):
                gate_second(ref.low_rim[1 - index], ref.low_corner[1 - index], index, 2 + index)
        for index in range(2):
            place = inner(index)
            gate_second(ref.second_zero[place], side_of(index), 2 + index, index)
        order = (2, 3, 0, 1)
        for index in range(2):
            if index == 0 and paired:
                taps_two[0] = jnp.zeros_like(taps_two[0])
                continue
            hidden = jnp.zeros((wide, merged), F32)
            for depth in range(3):
                hidden = hidden + jnp.dot(
                    taps_one[order[index + 2 - depth]],
                    mixer_at(ref.mixer_second, depth),
                    preferred_element_type=F32,
                )
            if index == 0:
                gate_first(hidden, ref.low_rim[2], ref.low_corner[0], index, index)
            else:
                gate_first(hidden, ref.first_zero[0], side_of(0), index, index)

    first_sphere = step * (UNROLL * GROUP)
    for part in range(UNROLL):
        base = first_sphere + part * GROUP
        slot = part * GROUP
        final = last if part == UNROLL - 1 else None
        earlier = ((part - 1) % UNROLL) * GROUP
        for index in range(2):
            sphere = base + 2 + index
            gate_second(
                gated(sphere, first_sphere + 2), side_of(sphere), slot + index, slot + 2 + index
            )
        pair = conv(taps_one, ref.mixer_second, slot)
        for index in range(2):
            sphere = base + 1 + index
            saved = ref.first[inside(sphere, first_sphere + 1, ref.first.shape[0])]
            gate_first(pair[index], saved, side_of(sphere), slot + index, slot + 2 + index)
        for index in range(2):
            sphere = base + 4 + index
            grad, side = gated(sphere, first_sphere + 2), side_of(sphere)
            if final is not None:
                grad = jnp.where(final, ref.high_rim[index], grad)
                side = jnp.where(final, ref.high_corner[index], side)
            gate_second(grad, side, slot + 2 + index, slot + 4 + index)
        mix_rows(ref.spread, earlier)
        pair = conv(taps_one, ref.mixer_second, slot + 2)
        for index in range(2):
            sphere = base + 3 + index
            saved = ref.first[inside(sphere, first_sphere + 1, ref.first.shape[0])]
            side = side_of(sphere)
            if final is not None and index == 1:
                saved = jnp.where(final, ref.high_rim[2], saved)
                side = jnp.where(final, ref.high_corner[0], side)
            gate_first(pair[index], saved, side, slot + 2 + index, slot + 4 + index)
        for start in range(0, GROUP, 2):
            pair = conv(taps_two, ref.mixer_first, slot + start)
            for index in range(2):
                volume[slot + start + index] = pair[index].astype(BF16)
            warp_columns(ref.tap_rows, start * cameras // GROUP, (start + 2) * cameras // GROUP)
        ref.spread[...] = spread_rows(step * UNROLL + part)
        ref.tap_rows[...] = tap_rows(step * UNROLL + part)
    for slot in range(2):
        taps_two[slot] = taps_two[slot + UNROLL * GROUP]

    def joined(row):
        return jnp.concatenate(
            [
                total[camera, :, row * channels : (row + 1) * channels]
                for camera in range(cameras)
            ],
            axis=1,
        )

    @pl.when(last)
    def _():
        mix_rows(ref.spread, (UNROLL - 1) * GROUP)
        warp_columns(ref.tap_rows, 0, cameras)
        if not paired:
            for row in range(row_count):
                ref.whole[row] = joined(row)
            return
        half = row_count // 2
        own_high = ref.info[1] > 0
        for row in range(half):
            low, high = joined(row), joined(row + half)
            for mine, main, left, right in (
                (True, ref.own, ref.own_left, ref.own_right),
                (False, ref.peer, ref.peer_left, ref.peer_right),
            ):
                value = jnp.where(own_high, high, low) if mine else jnp.where(own_high, low, high)
                main[row] = value[LEFT : LEFT + columns].astype(main.dtype)
                left[row] = value[:LEFT].astype(BF16)
                right[row] = value[LEFT + columns :].astype(BF16)


def sweep(info, volumes, tables, row_count, cameras, paired):
    second, first = volumes
    spheres, columns, merged = second.shape
    groups = spheres // GROUP
    wide = columns + 16
    extended = columns + LEFT + RIGHT
    channels = merged // row_count
    half, lanes = row_count // 2, cameras * channels
    once = pl.Buffered(buffer_count=1)

    def whole(shape):
        zeros = (0,) * len(shape)
        return pl.BlockSpec(shape, lambda g, s: zeros, pipeline_mode=once)

    def spheres_from(ahead, count, **more):
        def index_map(g, s):
            return block_start(s[0], ahead(g), count, spheres), 0, 0

        shape = (pl.Element(count), pl.Element(columns), pl.Element(merged))
        return pl.BlockSpec(shape, index_map, **more)

    block = UNROLL * GROUP
    inputs = {name: (array, whole(array.shape)) for name, array in tables.items()}
    inputs.update(
        second=(second, spheres_from(lambda g: block * g + 2, block)),
        first=(first, spheres_from(lambda g: block * g + 1, block)),
        second_zero=(second, spheres_from(lambda g: 0, 2, pipeline_mode=once)),
        first_zero=(first, spheres_from(lambda g: 0, 1, pipeline_mode=once)),
    )
    if paired:
        outputs = dict(
            own=((half, columns, lanes), F32),
            own_left=((half, LEFT, lanes), BF16),
            own_right=((half, RIGHT, lanes), BF16),
            peer=((half, columns, lanes), BF16),
            peer_left=((half, LEFT, lanes), BF16),
            peer_right=((half, RIGHT, lanes), BF16),
        )
    else:
        outputs = dict(whole=((row_count, extended, lanes), F32))
    scratch = dict(
        taps_one=((GROUP, wide, 3 * merged), BF16),
        taps_two=((block + 2, columns, 3 * merged), BF16),
        padded_one=((block, columns + 32, merged), F32),
        padded_two=((block, wide, merged), F32),
        volume=((block, columns, merged), BF16),
        mixed=((cameras, columns // VBLOCK, GROUP * VBLOCK, merged), BF16),
        total=((cameras, extended, merged), F32),
        expand=((cameras * row_count * row_count, merged), BF16),
        spread=((GROUP * cameras * row_count, merged), F32),
        tap_rows=((cameras * SLOT, GROUP * VBLOCK), F32),
    )
    names = list(dict(info=0)) + list(inputs) + list(outputs) + list(scratch)
    flops = 2 * spheres * columns * merged * merged * (18 + cameras + cameras // 2)
    results = pl.pallas_call(
        functools.partial(sweep_kernel, names, row_count, paired),
        grid_spec=pltpu.PrefetchScalarGridSpec(
            num_scalar_prefetch=1,
            grid=(groups // UNROLL,),
            in_specs=[spec for _, spec in inputs.values()],
            out_specs=[whole(shape) for shape, _ in outputs.values()],
            scratch_shapes=[pltpu.VMEM(shape, kind) for shape, kind in scratch.values()],
        ),
        out_shape=[jax.ShapeDtypeStruct(shape, kind) for shape, kind in outputs.values()],
        compiler_params=pltpu.CompilerParams(
            dimension_semantics=(pltpu.ARBITRARY,), vmem_limit_bytes=36 * 2**20
        ),
        cost_estimate=pl.CostEstimate(
            flops=flops, bytes_accessed=2 * second.size * 2, transcendentals=0
        ),
        name="sweep",
    )(info, *[array for array, _ in inputs.values()])
    return SimpleNamespace(**dict(zip(outputs, results)))


def finish_kernel(own, peer, own_start, own_end, peer_start, peer_end, out):
    columns = out.shape[1]
    out[...] = own[...] + peer[...].astype(F32)
    start, end = slice(0, RIGHT), slice(columns - LEFT, columns)
    out[:, start] = out[:, start] + (own_start[...].astype(F32) + peer_start[...].astype(F32))
    out[:, end] = out[:, end] + (own_end[...].astype(F32) + peer_end[...].astype(F32))


def row_mixers(kernel, row_count):
    channels = kernel.shape[3]
    strip = jnp.transpose(kernel, (0, 1, 4, 2, 3)).reshape(9, channels, 3 * channels)
    merged = row_count * channels
    strip = jnp.pad(strip, ((0, 0), (0, 0), (merged, merged)))
    rows = [
        lax.slice_in_dim(
            strip, merged - (row - 1) * channels, 2 * merged - (row - 1) * channels, axis=2
        )
        for row in range(row_count)
    ]
    return jnp.stack(rows, axis=1).reshape(3, 3 * merged, merged)


def ring(offset):
    count = lax.axis_size("azim")
    return [(i, (i + offset) % count) for i in range(count)]


def stride(offset):
    count = lax.axis_size("depth")
    if count == 2:
        return [(0, 1), (1, 0)]
    return [(i, i + offset) for i in range(count) if 0 <= i + offset < count]


def joint(depth_pairs, azim_pairs):
    width = lax.axis_size("azim")
    return [
        (d0 * width + a0, d1 * width + a1)
        for d0, d1 in depth_pairs
        for a0, a1 in azim_pairs
    ]


def body(cot, second, first, kernel_first, kernel_second, row_resample, col_taps, band_width, col_offset):
    spheres, columns, merged = cot.shape
    cameras, _, row_count, _ = row_resample.shape
    depth_index = lax.axis_index("depth").astype(jnp.int32)
    paired = lax.axis_size("depth") == 2
    both = ("depth", "azim")
    forward, backward = ring(1), ring(-1)
    tables = {}

    def send(offset, side):
        right, rim, corner = edges(jnp.full((1,), side, jnp.int32), cot, second, first)
        pairs = stride(offset)
        got_rim = lax.ppermute(rim, "depth", pairs)
        return right, got_rim, lax.ppermute(corner, both, joint(pairs, forward))

    if paired:
        right, high_rim, high_corner = send(-1, 1 - depth_index)
        flip = depth_index
    else:
        right, low_rim, low_corner = send(1, 1)
        _, high_rim, high_corner = send(-1, 0)
        tables.update(low_rim=low_rim, low_corner=low_corner)
        flip = jnp.zeros((), jnp.int32)
    info = jnp.stack([flip, depth_index])
    turned = lambda kernel: jnp.where(flip > 0, kernel[::-1], kernel)

    keep = lax.broadcasted_iota(jnp.int32, col_taps.shape, 2) < band_width[:, :, None]
    taps = jnp.where(keep, col_taps, 0.0)
    table = jnp.concatenate([taps, col_offset[:, :, None].astype(F32)], axis=2)
    table = jnp.pad(jnp.transpose(table, (0, 2, 1)), ((0, 0), (0, SLOT - TAPS - 1), (0, 0)))
    tables.update(
        high_rim=high_rim,
        high_corner=high_corner,
        from_left=lax.ppermute(right, "azim", forward),
        mixer_second=row_mixers(turned(kernel_second), row_count),
        mixer_first=row_mixers(turned(kernel_first), row_count),
        row_table=jnp.transpose(row_resample, (1, 0, 2, 3)).reshape(spheres, 1, -1),
        tap_table=table.reshape(cameras * SLOT, spheres).astype(BF16),
    )
    second_grad = gate_all(cot, second)
    parts = sweep(info, (second_grad, first), tables, row_count, cameras, paired)

    if paired:
        swap = stride(1)
        got = (
            lax.ppermute(parts.peer, "depth", swap),
            lax.ppermute(parts.own_right, "azim", forward),
            lax.ppermute(parts.own_left, "azim", backward),
            lax.ppermute(parts.peer_right, both, joint(swap, forward)),
            lax.ppermute(parts.peer_left, both, joint(swap, backward)),
        )
        return pl.pallas_call(
            finish_kernel,
            out_shape=jax.ShapeDtypeStruct(parts.own.shape, F32),
            name="finish",
        )(parts.own, *got)
    partial = parts.whole
    at_end = lax.ppermute(partial[:, :LEFT], "azim", backward)
    at_start = lax.ppermute(partial[:, columns + LEFT :], "azim", forward)
    inner = partial[:, LEFT : columns + LEFT]
    inner = inner.at[:, columns - LEFT :].add(at_end)
    inner = inner.at[:, :RIGHT].add(at_start)
    return lax.psum_scatter(inner, "depth", scatter_dimension=0, tiled=True)


def solution(mesh):
    placed = (
        P("depth", "azim", None),
        P("depth", "azim", None),
        P("depth", "azim", None),
        P(),
        P(),
        P(None, "depth", None, None),
        P(None, "depth", None),
        P(None, "depth"),
        P(None, "depth"),
    )
    return jax.shard_map(
        body, mesh=mesh, in_specs=placed, out_specs=P("depth", "azim", None), check_vma=False
    )
```

```python
import functools
from types import SimpleNamespace

import jax
import jax.numpy as jnp
from jax import lax
from jax.experimental import pallas as pl
from jax.experimental.pallas import tpu as pltpu
from jax.sharding import PartitionSpec as P

TAPS = 8
SHIFT = 24
HALO = 4
LEAD = 2
LEFT = 40
RIGHT = 24
GROUP = 4
VBLOCK = 64
WINDOW = VBLOCK + LEFT + RIGHT
SLOT = 16
UNROLL = 1
BF16 = jnp.bfloat16
F32 = jnp.float32


def rim_kernel(side, cot_rim, second_rim, first_rim, rim):
    top = side[0]
    for index in range(2):
        place = top + (1 - 2 * top) * index
        cot, saved = cot_rim[place], second_rim[place]
        rim[index] = jnp.where(saved > 0, cot, jnp.zeros_like(cot))
    rim[2] = first_rim[0]


def edge_kernel(side, cot_right, second_right, first_right, rim, right, corner):
    del rim
    spheres = cot_right.shape[0]
    top = side[0]
    last = slice(8 - HALO, 8)
    cot, saved = cot_right[:, last], second_right[:, last]
    right[:, 0:HALO] = jnp.where(saved > 0, cot, jnp.zeros_like(cot))
    right[:, HALO : 2 * HALO] = first_right[:, last]
    for index in range(2):
        corner[index] = right[top * (spheres - 1) + (1 - 2 * top) * index]


def edges(side, cot, second, first):
    spheres, columns, merged = cot.shape
    pairs = spheres // 2
    high = pl.BlockSpec((spheres, 8, merged), lambda g, s: (0, columns // 8 - 1, 0))
    pair = pl.BlockSpec((2, columns, merged), lambda g, s: (s[0] * (pairs - 1), 0, 0))
    one = pl.BlockSpec((1, columns, merged), lambda g, s: (s[0] * (spheres - 1), 0, 0))

    def call(kernel, in_specs, shapes, name):
        return pl.pallas_call(
            kernel,
            grid_spec=pltpu.PrefetchScalarGridSpec(
                num_scalar_prefetch=1,
                grid=(1,),
                in_specs=in_specs,
                out_specs=[pl.BlockSpec(s, lambda g, s: (0, 0, 0)) for s in shapes],
            ),
            out_shape=[jax.ShapeDtypeStruct(s, BF16) for s in shapes],
            name=name,
        )

    rim_shape = (3, columns, merged)
    (rim,) = call(rim_kernel, [pair, pair, one], (rim_shape,), "rim")(side, cot, second, first)
    shapes = ((spheres, 2 * HALO, merged), (2, 2 * HALO, merged))
    token = pl.BlockSpec((1, 8, merged), lambda g, s: (0, 0, 0))
    right, corner = call(edge_kernel, [high, high, high, token], shapes, "edges")(
        side, cot, second, first, rim
    )
    return right, rim, corner


def gate_kernel(cot, second, out):
    size = cot.shape[0]
    place = pl.ds(pl.program_id(0) * size, size)
    out[place] = jnp.where(second[...] > 0, cot[...], jnp.zeros_like(cot))


def gate_all(cot, second):
    spheres, columns, merged = cot.shape
    block = pl.BlockSpec((4 * GROUP, columns, merged), lambda g: (g, 0, 0))
    return pl.pallas_call(
        gate_kernel,
        grid=(spheres // (4 * GROUP),),
        in_specs=[block, block],
        out_specs=pl.BlockSpec(memory_space=pltpu.VMEM),
        out_shape=pltpu.VMEM(cot.shape, BF16),
        compiler_params=pltpu.CompilerParams(vmem_limit_bytes=44 * 2**20),
        cost_estimate=pl.CostEstimate(
            flops=cot.size, bytes_accessed=6 * cot.size, transcendentals=0
        ),
        name="gate",
    )(cot, second)


def block_start(flip, sphere, count, spheres):
    sphere = jnp.minimum(sphere, spheres - count)
    return sphere + flip * (spheres - count - 2 * sphere)


def sweep_kernel(names, row_count, paired, *refs):
    ref = SimpleNamespace(**dict(zip(names, refs)))
    flip = ref.info[0]
    step = pl.program_id(0)
    last = step == pl.num_programs(0) - 1
    spheres, _, merged = ref.from_left.shape
    taps_one, taps_two = ref.taps_one, ref.taps_two
    columns = taps_two.shape[1]
    volume, mixed, total = ref.volume, ref.mixed, ref.total
    cameras = total.shape[0]
    channels = merged // row_count
    wide = columns + 16
    blocks = columns // VBLOCK
    actual = lambda v: flip * (spheres - 1) + (1 - 2 * flip) * v
    inner = lambda i: flip + (1 - 2 * flip) * i
    mixer_at = lambda mixers, depth: mixers[depth]

    def store_taps(source, target, slot, first_row, rows):
        for tap in range(3):
            target[slot % target.shape[0], :, tap * merged : (tap + 1) * merged] = source[
                first_row - tap : first_row - tap + rows
            ].astype(BF16)

    def gate_second(grad, side, index, slot):
        padded = ref.padded_one.at[index]
        padded[16 : 16 + columns] = grad.astype(F32)
        padded[16 - HALO : 16] = side[0:HALO].astype(F32)
        store_taps(padded, taps_one, slot, 9, wide)

    def gated(v, first_sphere):
        return ref.second[inside(v, first_sphere, ref.second.shape[0])]

    def inside(v, first_sphere, count):
        start = block_start(flip, first_sphere, count, spheres)
        return actual(jnp.minimum(v, spheres - 1)) - start

    def side_of(v):
        return ref.from_left[actual(jnp.minimum(v, spheres - 1))]

    def conv(source, mixers, slot):
        value = None
        for depth in (2, 1, 0):
            lhs = jnp.concatenate(
                [source[(slot + at - depth) % source.shape[0]] for at in (2, 3)], axis=0
            )
            part = jnp.dot(lhs, mixer_at(mixers, depth), preferred_element_type=F32)
            value = part if value is None else value + part
        rows = source.shape[1]
        return value[:rows], value[rows:]

    def gate_first(hidden, saved, side, index, slot):
        low = side.astype(F32)
        keep = jnp.concatenate([low, saved.astype(F32), low], axis=0) > 0
        ref.padded_two[index] = jnp.where(keep, hidden, 0.0)
        store_taps(ref.padded_two.at[index], taps_two, slot, 9 - LEAD, columns)

    lane = lax.broadcasted_iota(jnp.int32, (channels, merged), 1)
    sub = lax.broadcasted_iota(jnp.int32, (channels, merged), 0)
    diagonal = lax.rem(lane, channels) == sub
    table_lanes = cameras * row_count * row_count
    owner = lax.broadcasted_iota(
        jnp.int32, (cameras * row_count, table_lanes), 1
    ) // row_count == lax.broadcasted_iota(jnp.int32, (cameras * row_count, table_lanes), 0)

    def spread_rows(group):
        rows = [
            jnp.where(owner, ref.row_table[actual(group * GROUP + sphere)], 0.0)
            for sphere in range(GROUP)
        ]
        return jnp.dot(
            jnp.concatenate(rows, axis=0).astype(BF16),
            ref.expand[...],
            preferred_element_type=F32,
        )

    def mix_rows(spread, earlier):
        for camera in range(cameras):
            for sphere in range(GROUP):
                start = (sphere * cameras + camera) * row_count
                weights = jnp.concatenate(
                    [
                        jnp.where(diagonal, spread[start + r : start + r + 1], 0.0)
                        for r in range(row_count)
                    ],
                    axis=0,
                ).astype(BF16)
                value = jnp.dot(
                    volume[earlier + sphere], weights, preferred_element_type=F32
                ).astype(BF16)
                for block in range(blocks):
                    mixed[camera, block, sphere * VBLOCK : (sphere + 1) * VBLOCK] = value[
                        block * VBLOCK : (block + 1) * VBLOCK
                    ]

    width = GROUP * VBLOCK
    distance = (
        lax.rem(lax.broadcasted_iota(jnp.int32, (WINDOW, width), 1), VBLOCK)
        - lax.broadcasted_iota(jnp.int32, (WINDOW, width), 0)
        + (LEFT - LEAD)
    ).astype(F32)

    def tap_rows(group):
        quarter = lax.broadcasted_iota(jnp.int32, (spheres, width), 1) // VBLOCK
        chosen = lax.broadcasted_iota(jnp.int32, (spheres, width), 0) == actual(
            group * GROUP + quarter
        )
        return jnp.dot(
            ref.tap_table[...], chosen.astype(BF16), preferred_element_type=F32
        )

    def warp_columns(rows_all, first, last):
        for camera in range(first, last):
            rows = rows_all[camera * SLOT : (camera + 1) * SLOT]
            tap_of = distance - rows[TAPS : TAPS + 1]
            matrix = jnp.zeros((WINDOW, width), F32)
            for tap in range(TAPS):
                matrix = jnp.where(tap_of == float(tap), rows[tap : tap + 1], matrix)
            matrix = matrix.astype(BF16)
            for block in range(blocks):
                place = slice(block * VBLOCK, block * VBLOCK + WINDOW)
                total[camera, place] = total[camera, place] + jnp.dot(
                    matrix, mixed[camera, block], preferred_element_type=F32
                )

    @pl.when(step == 0)
    def _():
        from_table = lax.broadcasted_iota(jnp.int32, (table_lanes, merged), 0)
        to_lane = lax.broadcasted_iota(jnp.int32, (table_lanes, merged), 1)
        ref.expand[...] = jnp.where(
            lax.rem(from_table, row_count) == to_lane // channels, 1.0, 0.0
        ).astype(BF16)
        total[...] = jnp.zeros_like(total)
        volume[...] = jnp.zeros_like(volume)
        ref.spread[...] = jnp.zeros_like(ref.spread)
        ref.tap_rows[...] = jnp.zeros_like(ref.tap_rows)
        if paired:
            taps_one[2] = jnp.zeros_like(taps_one[2])
            taps_one[3] = jnp.zeros_like(taps_one[3])
        else:
            for index in range(2):
                gate_second(ref.low_rim[1 - index], ref.low_corner[1 - index], index, 2 + index)
        for index in range(2):
            place = inner(index)
            gate_second(ref.second_zero[place], side_of(index), 2 + index, index)
        order = (2, 3, 0, 1)
        for index in range(2):
            if index == 0 and paired:
                taps_two[0] = jnp.zeros_like(taps_two[0])
                continue
            hidden = jnp.zeros((wide, merged), F32)
            for depth in range(3):
                hidden = hidden + jnp.dot(
                    taps_one[order[index + 2 - depth]],
                    mixer_at(ref.mixer_second, depth),
                    preferred_element_type=F32,
                )
            if index == 0:
                gate_first(hidden, ref.low_rim[2], ref.low_corner[0], index, index)
            else:
                gate_first(hidden, ref.first_zero[0], side_of(0), index, index)

    first_sphere = step * (UNROLL * GROUP)
    for part in range(UNROLL):
        base = first_sphere + part * GROUP
        slot = part * GROUP
        final = last if part == UNROLL - 1 else None
        earlier = ((part - 1) % UNROLL) * GROUP
        for index in range(2):
            sphere = base + 2 + index
            gate_second(
                gated(sphere, first_sphere + 2), side_of(sphere), slot + index, slot + 2 + index
            )
        pair = conv(taps_one, ref.mixer_second, slot)
        for index in range(2):
            sphere = base + 1 + index
            saved = ref.first[inside(sphere, first_sphere + 1, ref.first.shape[0])]
            gate_first(pair[index], saved, side_of(sphere), slot + index, slot + 2 + index)
        for index in range(2):
            sphere = base + 4 + index
            grad, side = gated(sphere, first_sphere + 2), side_of(sphere)
            if final is not None:
                grad = jnp.where(final, ref.high_rim[index], grad)
                side = jnp.where(final, ref.high_corner[index], side)
            gate_second(grad, side, slot + 2 + index, slot + 4 + index)
        mix_rows(ref.spread, earlier)
        pair = conv(taps_one, ref.mixer_second, slot + 2)
        for index in range(2):
            sphere = base + 3 + index
            saved = ref.first[inside(sphere, first_sphere + 1, ref.first.shape[0])]
            side = side_of(sphere)
            if final is not None and index == 1:
                saved = jnp.where(final, ref.high_rim[2], saved)
                side = jnp.where(final, ref.high_corner[0], side)
            gate_first(pair[index], saved, side, slot + 2 + index, slot + 4 + index)
        for start in range(0, GROUP, 2):
            pair = conv(taps_two, ref.mixer_first, slot + start)
            for index in range(2):
                volume[slot + start + index] = pair[index].astype(BF16)
            warp_columns(ref.tap_rows, start * cameras // GROUP, (start + 2) * cameras // GROUP)
        ref.spread[...] = spread_rows(step * UNROLL + part)
        ref.tap_rows[...] = tap_rows(step * UNROLL + part)
    for slot in range(2):
        taps_two[slot] = taps_two[slot + UNROLL * GROUP]

    def joined(row):
        return jnp.concatenate(
            [
                total[camera, :, row * channels : (row + 1) * channels]
                for camera in range(cameras)
            ],
            axis=1,
        )

    @pl.when(last)
    def _():
        mix_rows(ref.spread, (UNROLL - 1) * GROUP)
        warp_columns(ref.tap_rows, 0, cameras)
        if not paired:
            for row in range(row_count):
                ref.whole[row] = joined(row)
            return
        half = row_count // 2
        own_high = ref.info[1] > 0
        for row in range(half):
            low, high = joined(row), joined(row + half)
            for mine, main, left, right in (
                (True, ref.own, ref.own_left, ref.own_right),
                (False, ref.peer, ref.peer_left, ref.peer_right),
            ):
                value = jnp.where(own_high, high, low) if mine else jnp.where(own_high, low, high)
                main[row] = value[LEFT : LEFT + columns].astype(main.dtype)
                left[row] = value[:LEFT].astype(BF16)
                right[row] = value[LEFT + columns :].astype(BF16)


def sweep(info, volumes, tables, row_count, cameras, paired):
    second, first = volumes
    spheres, columns, merged = second.shape
    groups = spheres // GROUP
    wide = columns + 16
    extended = columns + LEFT + RIGHT
    channels = merged // row_count
    half, lanes = row_count // 2, cameras * channels
    once = pl.Buffered(buffer_count=1)

    def whole(shape):
        zeros = (0,) * len(shape)
        return pl.BlockSpec(shape, lambda g, s: zeros, pipeline_mode=once)

    def spheres_from(ahead, count, **more):
        def index_map(g, s):
            return block_start(s[0], ahead(g), count, spheres), 0, 0

        shape = (pl.Element(count), pl.Element(columns), pl.Element(merged))
        return pl.BlockSpec(shape, index_map, **more)

    block = UNROLL * GROUP
    inputs = {name: (array, whole(array.shape)) for name, array in tables.items()}
    inputs.update(
        second=(second, spheres_from(lambda g: block * g + 2, block)),
        first=(first, spheres_from(lambda g: block * g + 1, block)),
        second_zero=(second, spheres_from(lambda g: 0, 2, pipeline_mode=once)),
        first_zero=(first, spheres_from(lambda g: 0, 1, pipeline_mode=once)),
    )
    if paired:
        outputs = dict(
            own=((half, columns, lanes), F32),
            own_left=((half, LEFT, lanes), BF16),
            own_right=((half, RIGHT, lanes), BF16),
            peer=((half, columns, lanes), BF16),
            peer_left=((half, LEFT, lanes), BF16),
            peer_right=((half, RIGHT, lanes), BF16),
        )
    else:
        outputs = dict(whole=((row_count, extended, lanes), F32))
    scratch = dict(
        taps_one=((GROUP, wide, 3 * merged), BF16),
        taps_two=((block + 2, columns, 3 * merged), BF16),
        padded_one=((block, columns + 32, merged), F32),
        padded_two=((block, wide, merged), F32),
        volume=((block, columns, merged), BF16),
        mixed=((cameras, columns // VBLOCK, GROUP * VBLOCK, merged), BF16),
        total=((cameras, extended, merged), F32),
        expand=((cameras * row_count * row_count, merged), BF16),
        spread=((GROUP * cameras * row_count, merged), F32),
        tap_rows=((cameras * SLOT, GROUP * VBLOCK), F32),
    )
    names = list(dict(info=0)) + list(inputs) + list(outputs) + list(scratch)
    flops = 2 * spheres * columns * merged * merged * (18 + cameras + cameras // 2)
    results = pl.pallas_call(
        functools.partial(sweep_kernel, names, row_count, paired),
        grid_spec=pltpu.PrefetchScalarGridSpec(
            num_scalar_prefetch=1,
            grid=(groups // UNROLL,),
            in_specs=[spec for _, spec in inputs.values()],
            out_specs=[whole(shape) for shape, _ in outputs.values()],
            scratch_shapes=[pltpu.VMEM(shape, kind) for shape, kind in scratch.values()],
        ),
        out_shape=[jax.ShapeDtypeStruct(shape, kind) for shape, kind in outputs.values()],
        compiler_params=pltpu.CompilerParams(
            dimension_semantics=(pltpu.ARBITRARY,), vmem_limit_bytes=36 * 2**20
        ),
        cost_estimate=pl.CostEstimate(
            flops=flops, bytes_accessed=2 * second.size * 2, transcendentals=0
        ),
        name="sweep",
    )(info, *[array for array, _ in inputs.values()])
    return SimpleNamespace(**dict(zip(outputs, results)))


def finish_kernel(own, peer, own_start, own_end, peer_start, peer_end, out):
    columns = out.shape[1]
    out[...] = own[...] + peer[...].astype(F32)
    start, end = slice(0, RIGHT), slice(columns - LEFT, columns)
    out[:, start] = out[:, start] + (own_start[...].astype(F32) + peer_start[...].astype(F32))
    out[:, end] = out[:, end] + (own_end[...].astype(F32) + peer_end[...].astype(F32))


def row_mixers(kernel, row_count):
    channels = kernel.shape[3]
    strip = jnp.transpose(kernel, (0, 1, 4, 2, 3)).reshape(9, channels, 3 * channels)
    merged = row_count * channels
    strip = jnp.pad(strip, ((0, 0), (0, 0), (merged, merged)))
    rows = [
        lax.slice_in_dim(
            strip, merged - (row - 1) * channels, 2 * merged - (row - 1) * channels, axis=2
        )
        for row in range(row_count)
    ]
    return jnp.stack(rows, axis=1).reshape(3, 3 * merged, merged)


def ring(offset):
    count = lax.axis_size("azim")
    return [(i, (i + offset) % count) for i in range(count)]


def stride(offset):
    count = lax.axis_size("depth")
    if count == 2:
        return [(0, 1), (1, 0)]
    return [(i, i + offset) for i in range(count) if 0 <= i + offset < count]


def joint(depth_pairs, azim_pairs):
    width = lax.axis_size("azim")
    return [
        (d0 * width + a0, d1 * width + a1)
        for d0, d1 in depth_pairs
        for a0, a1 in azim_pairs
    ]


def body(cot, second, first, kernel_first, kernel_second, row_resample, col_taps, band_width, col_offset):
    spheres, columns, merged = cot.shape
    cameras, _, row_count, _ = row_resample.shape
    depth_index = lax.axis_index("depth").astype(jnp.int32)
    paired = lax.axis_size("depth") == 2
    both = ("depth", "azim")
    forward, backward = ring(1), ring(-1)
    tables = {}

    def send(offset, side):
        right, rim, corner = edges(jnp.full((1,), side, jnp.int32), cot, second, first)
        pairs = stride(offset)
        got_rim = lax.ppermute(rim, "depth", pairs)
        return right, got_rim, lax.ppermute(corner, both, joint(pairs, forward))

    if paired:
        right, high_rim, high_corner = send(-1, 1 - depth_index)
        flip = depth_index
    else:
        right, low_rim, low_corner = send(1, 1)
        _, high_rim, high_corner = send(-1, 0)
        tables.update(low_rim=low_rim, low_corner=low_corner)
        flip = jnp.zeros((), jnp.int32)
    info = jnp.stack([flip, depth_index])
    turned = lambda kernel: jnp.where(flip > 0, kernel[::-1], kernel)

    keep = lax.broadcasted_iota(jnp.int32, col_taps.shape, 2) < band_width[:, :, None]
    taps = jnp.where(keep, col_taps, 0.0)
    table = jnp.concatenate([taps, col_offset[:, :, None].astype(F32)], axis=2)
    table = jnp.pad(jnp.transpose(table, (0, 2, 1)), ((0, 0), (0, SLOT - TAPS - 1), (0, 0)))
    tables.update(
        high_rim=high_rim,
        high_corner=high_corner,
        from_left=lax.ppermute(right, "azim", forward),
        mixer_second=row_mixers(turned(kernel_second), row_count),
        mixer_first=row_mixers(turned(kernel_first), row_count),
        row_table=jnp.transpose(row_resample, (1, 0, 2, 3)).reshape(spheres, 1, -1),
        tap_table=table.reshape(cameras * SLOT, spheres).astype(BF16),
    )
    second_grad = gate_all(cot, second)
    parts = sweep(info, (second_grad, first), tables, row_count, cameras, paired)

    if paired:
        swap = stride(1)
        got = (
            lax.ppermute(parts.peer, "depth", swap),
            lax.ppermute(parts.own_right, "azim", forward),
            lax.ppermute(parts.own_left, "azim", backward),
            lax.ppermute(parts.peer_right, both, joint(swap, forward)),
            lax.ppermute(parts.peer_left, both, joint(swap, backward)),
        )
        return pl.pallas_call(
            finish_kernel,
            out_shape=jax.ShapeDtypeStruct(parts.own.shape, F32),
            name="finish",
        )(parts.own, *got)
    partial = parts.whole
    at_end = lax.ppermute(partial[:, :LEFT], "azim", backward)
    at_start = lax.ppermute(partial[:, columns + LEFT :], "azim", forward)
    inner = partial[:, LEFT : columns + LEFT]
    inner = inner.at[:, columns - LEFT :].add(at_end)
    inner = inner.at[:, :RIGHT].add(at_start)
    return lax.psum_scatter(inner, "depth", scatter_dimension=0, tiled=True)


def solution(mesh):
    placed = (
        P("depth", "azim", None),
        P("depth", "azim", None),
        P("depth", "azim", None),
        P(),
        P(),
        P(None, "depth", None, None),
        P(None, "depth", None),
        P(None, "depth"),
        P(None, "depth"),
    )
    return jax.shard_map(
        body, mesh=mesh, in_specs=placed, out_specs=P("depth", "azim", None), check_vma=False
    )
```

```python
import functools
from types import SimpleNamespace

import jax
import jax.numpy as jnp
from jax import lax
from jax.experimental import pallas as pl
from jax.experimental.pallas import tpu as pltpu
from jax.sharding import PartitionSpec as P

TAPS = 8
SHIFT = 24
HALO = 4
LEAD = 2
LEFT = 40
RIGHT = 24
GROUP = 4
VBLOCK = 64
WINDOW = VBLOCK + LEFT + RIGHT
SLOT = 16
UNROLL = 1
BF16 = jnp.bfloat16
F32 = jnp.float32


def edge_kernel(
    side, cot_right, second_right, first_right, cot_rim, second_rim, first_rim, right, rim, corner
):
    spheres = cot_right.shape[0]
    gate = lambda cot, saved: jnp.where(saved > 0, cot, jnp.zeros_like(cot))
    top = side[0]
    for index in range(2):
        place = top + (1 - 2 * top) * index
        rim[index] = gate(cot_rim[place], second_rim[place])
    rim[2] = first_rim[0]
    last = slice(8 - HALO, 8)
    right[:, 0:HALO] = gate(cot_right[:, last], second_right[:, last])
    right[:, HALO : 2 * HALO] = first_right[:, last]
    for index in range(2):
        corner[index] = right[top * (spheres - 1) + (1 - 2 * top) * index]


def edges(side, cot, second, first):
    spheres, columns, merged = cot.shape
    pairs = spheres // 2
    high = pl.BlockSpec((spheres, 8, merged), lambda g, s: (0, columns // 8 - 1, 0))
    pair = pl.BlockSpec((2, columns, merged), lambda g, s: (s[0] * (pairs - 1), 0, 0))
    one = pl.BlockSpec((1, columns, merged), lambda g, s: (s[0] * (spheres - 1), 0, 0))
    shapes = ((spheres, 2 * HALO, merged), (3, columns, merged), (2, 2 * HALO, merged))
    return pl.pallas_call(
        edge_kernel,
        grid_spec=pltpu.PrefetchScalarGridSpec(
            num_scalar_prefetch=1,
            grid=(1,),
            in_specs=[high, high, high, pair, pair, one],
            out_specs=[pl.BlockSpec(s, lambda g, s: (0, 0, 0)) for s in shapes],
        ),
        out_shape=[jax.ShapeDtypeStruct(s, BF16) for s in shapes],
        name="edges",
    )(side, cot, second, first, cot, second, first)


def gate_kernel(cot, second, out):
    size = cot.shape[0]
    place = pl.ds(pl.program_id(0) * size, size)
    out[place] = jnp.where(second[...] > 0, cot[...], jnp.zeros_like(cot))


def gate_all(cot, second):
    spheres, columns, merged = cot.shape
    block = pl.BlockSpec((4 * GROUP, columns, merged), lambda g: (g, 0, 0))
    return pl.pallas_call(
        gate_kernel,
        grid=(spheres // (4 * GROUP),),
        in_specs=[block, block],
        out_specs=pl.BlockSpec(memory_space=pltpu.VMEM),
        out_shape=pltpu.VMEM(cot.shape, BF16),
        compiler_params=pltpu.CompilerParams(vmem_limit_bytes=44 * 2**20),
        cost_estimate=pl.CostEstimate(
            flops=cot.size, bytes_accessed=6 * cot.size, transcendentals=0
        ),
        name="gate",
    )(cot, second)


def block_start(flip, sphere, count, spheres):
    sphere = jnp.minimum(sphere, spheres - count)
    return sphere + flip * (spheres - count - 2 * sphere)


def sweep_kernel(names, row_count, paired, *refs):
    ref = SimpleNamespace(**dict(zip(names, refs)))
    flip = ref.info[0]
    step = pl.program_id(0)
    last = step == pl.num_programs(0) - 1
    spheres, _, merged = ref.from_left.shape
    taps_one, taps_two = ref.taps_one, ref.taps_two
    columns = taps_two.shape[1]
    volume, mixed, total = ref.volume, ref.mixed, ref.total
    cameras = total.shape[0]
    channels = merged // row_count
    wide = columns + 16
    blocks = columns // VBLOCK
    actual = lambda v: flip * (spheres - 1) + (1 - 2 * flip) * v
    inner = lambda i: flip + (1 - 2 * flip) * i
    mixer_at = lambda mixers, depth: mixers[depth]

    def store_taps(source, target, slot, first_row, rows):
        for tap in range(3):
            target[slot % target.shape[0], :, tap * merged : (tap + 1) * merged] = source[
                first_row - tap : first_row - tap + rows
            ].astype(BF16)

    def gate_second(grad, side, index, slot):
        padded = ref.padded_one.at[index]
        padded[16 : 16 + columns] = grad.astype(F32)
        padded[16 - HALO : 16] = side[0:HALO].astype(F32)
        store_taps(padded, taps_one, slot, 9, wide)

    def gated(v, first_sphere):
        return ref.second[inside(v, first_sphere, ref.second.shape[0])]

    def inside(v, first_sphere, count):
        start = block_start(flip, first_sphere, count, spheres)
        return actual(jnp.minimum(v, spheres - 1)) - start

    def side_of(v):
        return ref.from_left[actual(jnp.minimum(v, spheres - 1))]

    def conv(source, mixers, slot):
        value = None
        for depth in (2, 1, 0):
            lhs = jnp.concatenate(
                [source[(slot + at - depth) % source.shape[0]] for at in (2, 3)], axis=0
            )
            part = jnp.dot(lhs, mixer_at(mixers, depth), preferred_element_type=F32)
            value = part if value is None else value + part
        rows = source.shape[1]
        return value[:rows], value[rows:]

    def gate_first(hidden, saved, side, index, slot):
        low = side.astype(F32)
        keep = jnp.concatenate([low, saved.astype(F32), low], axis=0) > 0
        ref.padded_two[index] = jnp.where(keep, hidden, 0.0)
        store_taps(ref.padded_two.at[index], taps_two, slot, 9 - LEAD, columns)

    lane = lax.broadcasted_iota(jnp.int32, (channels, merged), 1)
    sub = lax.broadcasted_iota(jnp.int32, (channels, merged), 0)
    diagonal = lax.rem(lane, channels) == sub
    table_lanes = cameras * row_count * row_count
    owner = lax.broadcasted_iota(
        jnp.int32, (cameras * row_count, table_lanes), 1
    ) // row_count == lax.broadcasted_iota(jnp.int32, (cameras * row_count, table_lanes), 0)

    def spread_rows(group):
        rows = [
            jnp.where(owner, ref.row_table[actual(group * GROUP + sphere)], 0.0)
            for sphere in range(GROUP)
        ]
        return jnp.dot(
            jnp.concatenate(rows, axis=0).astype(BF16),
            ref.expand[...],
            preferred_element_type=F32,
        )

    def mix_rows(spread, earlier):
        for camera in range(cameras):
            for sphere in range(GROUP):
                start = (sphere * cameras + camera) * row_count
                weights = jnp.concatenate(
                    [
                        jnp.where(diagonal, spread[start + r : start + r + 1], 0.0)
                        for r in range(row_count)
                    ],
                    axis=0,
                ).astype(BF16)
                value = jnp.dot(
                    volume[earlier + sphere], weights, preferred_element_type=F32
                ).astype(BF16)
                for block in range(blocks):
                    mixed[camera, block, sphere * VBLOCK : (sphere + 1) * VBLOCK] = value[
                        block * VBLOCK : (block + 1) * VBLOCK
                    ]

    width = GROUP * VBLOCK
    distance = (
        lax.rem(lax.broadcasted_iota(jnp.int32, (WINDOW, width), 1), VBLOCK)
        - lax.broadcasted_iota(jnp.int32, (WINDOW, width), 0)
        + (LEFT - LEAD)
    ).astype(F32)

    def tap_rows(group):
        quarter = lax.broadcasted_iota(jnp.int32, (spheres, width), 1) // VBLOCK
        chosen = lax.broadcasted_iota(jnp.int32, (spheres, width), 0) == actual(
            group * GROUP + quarter
        )
        return jnp.dot(
            ref.tap_table[...], chosen.astype(BF16), preferred_element_type=F32
        )

    def warp_columns(rows_all, first, last):
        for camera in range(first, last):
            rows = rows_all[camera * SLOT : (camera + 1) * SLOT]
            tap_of = distance - rows[TAPS : TAPS + 1]
            matrix = jnp.zeros((WINDOW, width), F32)
            for tap in range(TAPS):
                matrix = jnp.where(tap_of == float(tap), rows[tap : tap + 1], matrix)
            matrix = matrix.astype(BF16)
            for block in range(blocks):
                place = slice(block * VBLOCK, block * VBLOCK + WINDOW)
                total[camera, place] = total[camera, place] + jnp.dot(
                    matrix, mixed[camera, block], preferred_element_type=F32
                )

    @pl.when(step == 0)
    def _():
        from_table = lax.broadcasted_iota(jnp.int32, (table_lanes, merged), 0)
        to_lane = lax.broadcasted_iota(jnp.int32, (table_lanes, merged), 1)
        ref.expand[...] = jnp.where(
            lax.rem(from_table, row_count) == to_lane // channels, 1.0, 0.0
        ).astype(BF16)
        total[...] = jnp.zeros_like(total)
        volume[...] = jnp.zeros_like(volume)
        ref.spread[...] = jnp.zeros_like(ref.spread)
        ref.tap_rows[...] = jnp.zeros_like(ref.tap_rows)
        if paired:
            taps_one[2] = jnp.zeros_like(taps_one[2])
            taps_one[3] = jnp.zeros_like(taps_one[3])
        else:
            for index in range(2):
                gate_second(ref.low_rim[1 - index], ref.low_corner[1 - index], index, 2 + index)
        for index in range(2):
            place = inner(index)
            gate_second(ref.second_zero[place], side_of(index), 2 + index, index)
        order = (2, 3, 0, 1)
        for index in range(2):
            if index == 0 and paired:
                taps_two[0] = jnp.zeros_like(taps_two[0])
                continue
            hidden = jnp.zeros((wide, merged), F32)
            for depth in range(3):
                hidden = hidden + jnp.dot(
                    taps_one[order[index + 2 - depth]],
                    mixer_at(ref.mixer_second, depth),
                    preferred_element_type=F32,
                )
            if index == 0:
                gate_first(hidden, ref.low_rim[2], ref.low_corner[0], index, index)
            else:
                gate_first(hidden, ref.first_zero[0], side_of(0), index, index)

    first_sphere = step * (UNROLL * GROUP)
    for part in range(UNROLL):
        base = first_sphere + part * GROUP
        slot = part * GROUP
        final = last if part == UNROLL - 1 else None
        earlier = ((part - 1) % UNROLL) * GROUP
        for index in range(2):
            sphere = base + 2 + index
            gate_second(
                gated(sphere, first_sphere + 2), side_of(sphere), slot + index, slot + 2 + index
            )
        pair = conv(taps_one, ref.mixer_second, slot)
        for index in range(2):
            sphere = base + 1 + index
            saved = ref.first[inside(sphere, first_sphere + 1, ref.first.shape[0])]
            gate_first(pair[index], saved, side_of(sphere), slot + index, slot + 2 + index)
        for index in range(2):
            sphere = base + 4 + index
            grad, side = gated(sphere, first_sphere + 2), side_of(sphere)
            if final is not None:
                grad = jnp.where(final, ref.high_rim[index], grad)
                side = jnp.where(final, ref.high_corner[index], side)
            gate_second(grad, side, slot + 2 + index, slot + 4 + index)
        mix_rows(ref.spread, earlier)
        pair = conv(taps_one, ref.mixer_second, slot + 2)
        for index in range(2):
            sphere = base + 3 + index
            saved = ref.first[inside(sphere, first_sphere + 1, ref.first.shape[0])]
            side = side_of(sphere)
            if final is not None and index == 1:
                saved = jnp.where(final, ref.high_rim[2], saved)
                side = jnp.where(final, ref.high_corner[0], side)
            gate_first(pair[index], saved, side, slot + 2 + index, slot + 4 + index)
        for start in range(0, GROUP, 2):
            pair = conv(taps_two, ref.mixer_first, slot + start)
            for index in range(2):
                volume[slot + start + index] = pair[index].astype(BF16)
            warp_columns(ref.tap_rows, start * cameras // GROUP, (start + 2) * cameras // GROUP)
        ref.spread[...] = spread_rows(step * UNROLL + part)
        ref.tap_rows[...] = tap_rows(step * UNROLL + part)
    for slot in range(2):
        taps_two[slot] = taps_two[slot + UNROLL * GROUP]

    def joined(row):
        return jnp.concatenate(
            [
                total[camera, :, row * channels : (row + 1) * channels]
                for camera in range(cameras)
            ],
            axis=1,
        )

    @pl.when(last)
    def _():
        mix_rows(ref.spread, (UNROLL - 1) * GROUP)
        warp_columns(ref.tap_rows, 0, cameras)
        if not paired:
            for row in range(row_count):
                ref.whole[row] = joined(row)
            return
        half = row_count // 2
        own_high = ref.info[1] > 0
        for row in range(half):
            low, high = joined(row), joined(row + half)
            for mine, main, left, right in (
                (True, ref.own, ref.own_left, ref.own_right),
                (False, ref.peer, ref.peer_left, ref.peer_right),
            ):
                value = jnp.where(own_high, high, low) if mine else jnp.where(own_high, low, high)
                main[row] = value[LEFT : LEFT + columns].astype(main.dtype)
                left[row] = value[:LEFT].astype(BF16)
                right[row] = value[LEFT + columns :].astype(BF16)


def sweep(info, volumes, tables, row_count, cameras, paired):
    second, first = volumes
    spheres, columns, merged = second.shape
    groups = spheres // GROUP
    wide = columns + 16
    extended = columns + LEFT + RIGHT
    channels = merged // row_count
    half, lanes = row_count // 2, cameras * channels
    once = pl.Buffered(buffer_count=1)

    def whole(shape):
        zeros = (0,) * len(shape)
        return pl.BlockSpec(shape, lambda g, s: zeros, pipeline_mode=once)

    def spheres_from(ahead, count, **more):
        def index_map(g, s):
            return block_start(s[0], ahead(g), count, spheres), 0, 0

        shape = (pl.Element(count), pl.Element(columns), pl.Element(merged))
        return pl.BlockSpec(shape, index_map, **more)

    block = UNROLL * GROUP
    inputs = {name: (array, whole(array.shape)) for name, array in tables.items()}
    inputs.update(
        second=(second, spheres_from(lambda g: block * g + 2, block)),
        first=(first, spheres_from(lambda g: block * g + 1, block)),
        second_zero=(second, spheres_from(lambda g: 0, 2, pipeline_mode=once)),
        first_zero=(first, spheres_from(lambda g: 0, 1, pipeline_mode=once)),
    )
    if paired:
        outputs = dict(
            own=((half, columns, lanes), F32),
            own_left=((half, LEFT, lanes), BF16),
            own_right=((half, RIGHT, lanes), BF16),
            peer=((half, columns, lanes), BF16),
            peer_left=((half, LEFT, lanes), BF16),
            peer_right=((half, RIGHT, lanes), BF16),
        )
    else:
        outputs = dict(whole=((row_count, extended, lanes), F32))
    scratch = dict(
        taps_one=((GROUP, wide, 3 * merged), BF16),
        taps_two=((block + 2, columns, 3 * merged), BF16),
        padded_one=((block, columns + 32, merged), F32),
        padded_two=((block, wide, merged), F32),
        volume=((block, columns, merged), BF16),
        mixed=((cameras, columns // VBLOCK, GROUP * VBLOCK, merged), BF16),
        total=((cameras, extended, merged), F32),
        expand=((cameras * row_count * row_count, merged), BF16),
        spread=((GROUP * cameras * row_count, merged), F32),
        tap_rows=((cameras * SLOT, GROUP * VBLOCK), F32),
    )
    names = list(dict(info=0)) + list(inputs) + list(outputs) + list(scratch)
    flops = 2 * spheres * columns * merged * merged * (18 + cameras + cameras // 2)
    results = pl.pallas_call(
        functools.partial(sweep_kernel, names, row_count, paired),
        grid_spec=pltpu.PrefetchScalarGridSpec(
            num_scalar_prefetch=1,
            grid=(groups // UNROLL,),
            in_specs=[spec for _, spec in inputs.values()],
            out_specs=[whole(shape) for shape, _ in outputs.values()],
            scratch_shapes=[pltpu.VMEM(shape, kind) for shape, kind in scratch.values()],
        ),
        out_shape=[jax.ShapeDtypeStruct(shape, kind) for shape, kind in outputs.values()],
        compiler_params=pltpu.CompilerParams(
            dimension_semantics=(pltpu.ARBITRARY,), vmem_limit_bytes=36 * 2**20
        ),
        cost_estimate=pl.CostEstimate(
            flops=flops, bytes_accessed=2 * second.size * 2, transcendentals=0
        ),
        name="sweep",
    )(info, *[array for array, _ in inputs.values()])
    return SimpleNamespace(**dict(zip(outputs, results)))


def finish_kernel(own, peer, own_start, own_end, peer_start, peer_end, out):
    columns = out.shape[1]
    out[...] = own[...] + peer[...].astype(F32)
    start, end = slice(0, RIGHT), slice(columns - LEFT, columns)
    out[:, start] = out[:, start] + (own_start[...].astype(F32) + peer_start[...].astype(F32))
    out[:, end] = out[:, end] + (own_end[...].astype(F32) + peer_end[...].astype(F32))


def row_mixers(kernel, row_count):
    channels = kernel.shape[3]
    strip = jnp.transpose(kernel, (0, 1, 4, 2, 3)).reshape(9, channels, 3 * channels)
    merged = row_count * channels
    strip = jnp.pad(strip, ((0, 0), (0, 0), (merged, merged)))
    rows = [
        lax.slice_in_dim(
            strip, merged - (row - 1) * channels, 2 * merged - (row - 1) * channels, axis=2
        )
        for row in range(row_count)
    ]
    return jnp.stack(rows, axis=1).reshape(3, 3 * merged, merged)


def ring(offset):
    count = lax.axis_size("azim")
    return [(i, (i + offset) % count) for i in range(count)]


def stride(offset):
    count = lax.axis_size("depth")
    if count == 2:
        return [(0, 1), (1, 0)]
    return [(i, i + offset) for i in range(count) if 0 <= i + offset < count]


def joint(depth_pairs, azim_pairs):
    width = lax.axis_size("azim")
    return [
        (d0 * width + a0, d1 * width + a1)
        for d0, d1 in depth_pairs
        for a0, a1 in azim_pairs
    ]


def body(cot, second, first, kernel_first, kernel_second, row_resample, col_taps, band_width, col_offset):
    spheres, columns, merged = cot.shape
    cameras, _, row_count, _ = row_resample.shape
    depth_index = lax.axis_index("depth").astype(jnp.int32)
    paired = lax.axis_size("depth") == 2
    both = ("depth", "azim")
    forward, backward = ring(1), ring(-1)
    tables = {}

    def send(offset, side):
        right, rim, corner = edges(jnp.full((1,), side, jnp.int32), cot, second, first)
        pairs = stride(offset)
        got_rim = lax.ppermute(rim, "depth", pairs)
        return right, got_rim, lax.ppermute(corner, both, joint(pairs, forward))

    if paired:
        right, high_rim, high_corner = send(-1, 1 - depth_index)
        flip = depth_index
    else:
        right, low_rim, low_corner = send(1, 1)
        _, high_rim, high_corner = send(-1, 0)
        tables.update(low_rim=low_rim, low_corner=low_corner)
        flip = jnp.zeros((), jnp.int32)
    info = jnp.stack([flip, depth_index])
    turned = lambda kernel: jnp.where(flip > 0, kernel[::-1], kernel)

    keep = lax.broadcasted_iota(jnp.int32, col_taps.shape, 2) < band_width[:, :, None]
    taps = jnp.where(keep, col_taps, 0.0)
    table = jnp.concatenate([taps, col_offset[:, :, None].astype(F32)], axis=2)
    table = jnp.pad(jnp.transpose(table, (0, 2, 1)), ((0, 0), (0, SLOT - TAPS - 1), (0, 0)))
    tables.update(
        high_rim=high_rim,
        high_corner=high_corner,
        from_left=lax.ppermute(right, "azim", forward),
        mixer_second=row_mixers(turned(kernel_second), row_count),
        mixer_first=row_mixers(turned(kernel_first), row_count),
        row_table=jnp.transpose(row_resample, (1, 0, 2, 3)).reshape(spheres, 1, -1),
        tap_table=table.reshape(cameras * SLOT, spheres).astype(BF16),
    )
    second_grad = gate_all(cot, second)
    parts = sweep(info, (second_grad, first), tables, row_count, cameras, paired)

    if paired:
        swap = stride(1)
        got = (
            lax.ppermute(parts.peer, "depth", swap),
            lax.ppermute(parts.own_right, "azim", forward),
            lax.ppermute(parts.own_left, "azim", backward),
            lax.ppermute(parts.peer_right, both, joint(swap, forward)),
            lax.ppermute(parts.peer_left, both, joint(swap, backward)),
        )
        return pl.pallas_call(
            finish_kernel,
            out_shape=jax.ShapeDtypeStruct(parts.own.shape, F32),
            name="finish",
        )(parts.own, *got)
    partial = parts.whole
    at_end = lax.ppermute(partial[:, :LEFT], "azim", backward)
    at_start = lax.ppermute(partial[:, columns + LEFT :], "azim", forward)
    inner = partial[:, LEFT : columns + LEFT]
    inner = inner.at[:, columns - LEFT :].add(at_end)
    inner = inner.at[:, :RIGHT].add(at_start)
    return lax.psum_scatter(inner, "depth", scatter_dimension=0, tiled=True)


def solution(mesh):
    placed = (
        P("depth", "azim", None),
        P("depth", "azim", None),
        P("depth", "azim", None),
        P(),
        P(),
        P(None, "depth", None, None),
        P(None, "depth", None),
        P(None, "depth"),
        P(None, "depth"),
    )
    return jax.shard_map(
        body, mesh=mesh, in_specs=placed, out_specs=P("depth", "azim", None), check_vma=False
    )
```
